128 devices in a mesh: data: 1, sp: 128 (over z, y, x, core).
Axes of the slice: x: 4, y: 4, z: 4, core: 2. Of those that a mesh axis runs over, the one named last changes fastest.
Arguments:
- latents: bfloat16 [1, 256, 256, 384], P('data', 'sp')
- cotangent: bfloat16 [1, 256, 256, 384], P('data', 'sp')
- ln_params: bfloat16 [2, 4, 384], replicated
- w_qkv: bfloat16 [2, 384, 1152], replicated
- w_out: bfloat16 [2, 6, 64, 384], replicated
- w_up: bfloat16 [2, 384, 1536], replicated
- w_down: bfloat16 [2, 1536, 384], replicated
Outputs:
- output 1: bfloat16 [1, 256, 256, 384], P('data', 'sp')
- output 2: bfloat16 [1, 256, 256, 384], P('data', 'sp')
- output 3: float32 [2, 4, 384], P('data')
- output 4: float32 [2, 384, 1152], P('data')
- output 5: float32 [2, 6, 64, 384], P('data')
- output 6: float32 [2, 384, 1536], P('data')
- output 7: float32 [2, 1536, 384], P('data')
All inputs are finite; a program needn't handle non-finite values.
Results may differ from the reference program's by a relative error of at most 0.02.
Values are sent between devices in bfloat16 or wider.
A program may use at most 1 GiB of HBM per device.

```python
import jax
import jax.numpy as jnp
from jax import lax

VIDEOS = 1
FRAMES = 256
PATCHES = 256
MODEL_WIDTH = 384
NUM_HEADS = 6
HEAD_DIM = MODEL_WIDTH // NUM_HEADS


def setup_inputs(seed: int = 0, part: int = 0) -> dict:
    part_key = jax.random.fold_in(jax.random.key(seed), part)
    key_x, key_cot = jax.random.split(part_key)
    key_ln, key_qkv, key_out, key_up, key_down = jax.random.split(jax.random.key(seed + 1), 5)
    act_shape = (VIDEOS, FRAMES, PATCHES, MODEL_WIDTH)
    ln_base = jnp.array([1.0, 0.0, 1.0, 0.0], dtype=jnp.float32)[None, :, None]
    ln_noise = jax.random.normal(key_ln, (2, 4, MODEL_WIDTH), jnp.float32)
    qkv_draw = jax.random.normal(key_qkv, (2, MODEL_WIDTH, 3 * MODEL_WIDTH), jnp.float32)
    out_draw = jax.random.normal(key_out, (2, NUM_HEADS, HEAD_DIM, MODEL_WIDTH), jnp.float32)
    up_draw = jax.random.normal(key_up, (2, MODEL_WIDTH, 4 * MODEL_WIDTH), jnp.float32)
    down_draw = jax.random.normal(key_down, (2, 4 * MODEL_WIDTH, MODEL_WIDTH), jnp.float32)
    return {
        'latents': jax.random.normal(key_x, act_shape, jnp.float32).astype(jnp.bfloat16),
        'cotangent': jax.random.normal(key_cot, act_shape, jnp.float32).astype(jnp.bfloat16),
        'ln_params': (ln_base + 0.25 * ln_noise).astype(jnp.bfloat16),
        'w_qkv': (1.25 * MODEL_WIDTH ** -0.5 * qkv_draw).astype(jnp.bfloat16),
        'w_out': (MODEL_WIDTH ** -0.5 * out_draw).astype(jnp.bfloat16),
        'w_up': (MODEL_WIDTH ** -0.5 * up_draw).astype(jnp.bfloat16),
        'w_down': ((4 * MODEL_WIDTH) ** -0.5 * down_draw).astype(jnp.bfloat16),
    }


def layer_norm(resid32, ln_gain, ln_shift):
    row_mean = jnp.mean(resid32, axis=-1, keepdims=True)
    centered = resid32 - row_mean
    variance = jnp.mean(centered * centered, axis=-1, keepdims=True)
    return (centered * lax.rsqrt(variance + 1e-6) * ln_gain + ln_shift).astype(jnp.bfloat16)


def attend_group(seq_group):
    queries = seq_group[:, :, 0].astype(jnp.float32)
    keys_all = seq_group[:, :, 1].astype(jnp.float32)
    values_all = seq_group[:, :, 2].astype(jnp.float32)
    scores = jnp.einsum('nlhe,nmhe->nhlm', queries, keys_all) * HEAD_DIM ** -0.5
    attn_probs = jax.nn.softmax(scores, axis=-1).astype(jnp.bfloat16)
    return jnp.einsum('nhlm,nmhe->nlhe', attn_probs.astype(jnp.float32), values_all).astype(jnp.bfloat16)


def attention(qkv_heads, lead_axis):
    lead_first = jnp.moveaxis(qkv_heads, lead_axis, 0)
    attended = lax.map(jax.checkpoint(attend_group), lead_first)
    return jnp.moveaxis(attended, 0, lead_axis).reshape(VIDEOS, FRAMES, PATCHES, MODEL_WIDTH)


def dit_block(block_in, ln_f32, w_qkv, w_out, w_up, w_down, lead_axis):
    block_in32 = block_in.astype(jnp.float32)
    a_in = layer_norm(block_in32, ln_f32[0], ln_f32[1])
    qkv_heads = jnp.einsum('btsd,de->btse', a_in.astype(jnp.float32), w_qkv).astype(jnp.bfloat16)
    qkv_heads = qkv_heads.reshape(VIDEOS, FRAMES, PATCHES, 3, NUM_HEADS, HEAD_DIM)
    attn_out = attention(qkv_heads, lead_axis)
    attn_proj = jnp.einsum('btsd,de->btse', attn_out.astype(jnp.float32), w_out.reshape(MODEL_WIDTH, MODEL_WIDTH))
    hid32 = (block_in32 + attn_proj).astype(jnp.bfloat16).astype(jnp.float32)
    m_in = layer_norm(hid32, ln_f32[2], ln_f32[3])
    up_proj = jnp.einsum('btsd,de->btse', m_in.astype(jnp.float32), w_up)
    act_out = jax.nn.gelu(up_proj, approximate=True).astype(jnp.bfloat16)
    mlp_down = jnp.einsum('btse,ed->btsd', act_out.astype(jnp.float32), w_down)
    return (hid32 + mlp_down).astype(jnp.bfloat16)


def reference(latents, cotangent, ln_params, w_qkv, w_out, w_up, w_down):
    weights32 = [weight.astype(jnp.float32) for weight in (ln_params, w_qkv, w_out, w_up, w_down)]

    def forward(block_in, ln_f32, qkv_f32, out_f32, up_f32, down_f32):
        mid_act = dit_block(block_in, ln_f32[0], qkv_f32[0], out_f32[0], up_f32[0], down_f32[0], 1)
        return dit_block(mid_act, ln_f32[1], qkv_f32[1], out_f32[1], up_f32[1], down_f32[1], 2)

    y_out, pullback = jax.vjp(forward, latents, *weights32)
    grads_all = pullback(cotangent)
    return (y_out, grads_all[0], grads_all[1], grads_all[2], grads_all[3], grads_all[4], grads_all[5])
```

```python
import functools

import jax
import jax.numpy as jnp
from jax import lax
from jax.experimental import pallas as pl
from jax.experimental.pallas import tpu as pltpu
from jax.sharding import PartitionSpec as P

F32 = jnp.float32
BF16 = jnp.bfloat16
D = 384
T = 512
SEQ = 256
FF = 1536
ROWS = 128
MESH = pl.DeviceIdType.MESH
VMEM_LIMIT = 60 * 1024 * 1024
GELU_C = 0.7978845608028654
GELU_A = 0.044715


def dot_nn(a, b):
    return lax.dot_general(a, b, (((1,), (0,)), ((), ())), preferred_element_type=F32)


def dot_nt(a, b):
    return lax.dot_general(a, b, (((1,), (1,)), ((), ())), preferred_element_type=F32)


def dot_tn(a, b):
    return lax.dot_general(a, b, (((0,), (0,)), ((), ())), preferred_element_type=F32)


def row_tiles(body):
    def step(i, _):
        body(pl.ds(pl.multiple_of(i * ROWS, ROWS), ROWS))
        return 0
    lax.fori_loop(0, T // ROWS, step, 0)


def ln_norm(x32):
    mean = jnp.sum(x32, axis=-1, keepdims=True) * (1.0 / D)
    centered = x32 - mean
    inv_std = lax.rsqrt(jnp.sum(centered * centered, axis=-1, keepdims=True) * (1.0 / D) + 1e-6)
    return centered * inv_std, inv_std


def ln_back(d32, normed, inv_std, gain):
    d_norm = d32 * gain
    d_center = d_norm - jnp.sum(d_norm, axis=-1, keepdims=True) * (1.0 / D)
    return inv_std * (d_center - normed * (jnp.sum(d_norm * normed, axis=-1, keepdims=True) * (1.0 / D)))


def head_pairs(body):
    def step(i, _):
        seq = i // 3
        pair = i - seq * 3
        rows = pl.ds(pl.multiple_of(seq * SEQ, SEQ), SEQ)
        body(i, rows, pair)
        return 0
    lax.fori_loop(0, 6, step, 0)


def pair_cols(which, pair):
    return pl.ds(pl.multiple_of(which * D + pair * 128, 128), 128)


def attn_forward(x_ref, ln_ref, wqkv_ref, qkv_s, p_s, o_s):
    def qkv_tile(rows):
        normed, _ = ln_norm(x_ref[rows, :].astype(F32))
        a_in = (normed * ln_ref[0:1, :] + ln_ref[1:2, :]).astype(BF16)
        qkv_s[rows, :] = dot_nn(a_in, wqkv_ref[...]).astype(BF16)
    row_tiles(qkv_tile)

    def heads(i, rows, pair):
        q2 = qkv_s[rows, pair_cols(0, pair)]
        k2 = qkv_s[rows, pair_cols(1, pair)]
        v2 = qkv_s[rows, pair_cols(2, pair)]
        outs = []
        for e in range(2):
            cut = slice(e * 64, e * 64 + 64)
            scores = dot_nt(q2[:, cut], k2[:, cut]) * 0.125
            top = jnp.max(scores, axis=-1, keepdims=True)
            expd = jnp.exp(scores - top)
            total = jnp.sum(expd, axis=-1, keepdims=True)
            probs = (expd * (1.0 / total)).astype(BF16)
            p_s[i * 2 + e] = probs
            outs.append(dot_nn(probs, v2[:, cut]).astype(BF16))
        o_s[rows, pair_cols(0, pair)] = jnp.concatenate(outs, axis=1)
    head_pairs(heads)


def hidden(x_ref, o_s, wout_ref, h_s, rows):
    hid = (x_ref[rows, :].astype(F32) + dot_nn(o_s[rows, :], wout_ref[...])).astype(BF16)
    h_s[rows, :] = hid
    return hid.astype(F32)


def gelu_parts(up):
    up2 = up * up
    tanh = jnp.tanh(GELU_C * up * (1.0 + GELU_A * up2))
    half = 0.5 + 0.5 * tanh
    return up2, tanh, half


def mlp_forward(hid32, ln_ref, wup_ref, wdown_ref):
    normed, _ = ln_norm(hid32)
    m_in = (normed * ln_ref[2:3, :] + ln_ref[3:4, :]).astype(BF16)
    total = None
    for c in range(4):
        up = dot_nn(m_in, wup_ref[:, c * D:(c + 1) * D])
        act = (up * gelu_parts(up)[2]).astype(BF16)
        part = dot_nn(act, wdown_ref[c * D:(c + 1) * D, :])
        total = part if total is None else total + part
    return (hid32 + total).astype(BF16)


def mlp_backward(hid32, dy, ln_ref, wup_ref, wout_ref, wdown_ref, m_s, act_s, dup_s, dhid_s, datt_s, lng_ref, rows, emit):
    normed, inv_std = ln_norm(hid32)
    m_in = (normed * ln_ref[2:3, :] + ln_ref[3:4, :]).astype(BF16)
    m_s[rows, :] = m_in
    total = None
    dm = None
    for c in range(4):
        cols = slice(c * D, (c + 1) * D)
        up = dot_nn(m_in, wup_ref[:, cols])
        up2, tanh, half = gelu_parts(up)
        act = (up * half).astype(BF16)
        act_s[rows, cols] = act
        if emit is not None:
            part = dot_nn(act, wdown_ref[cols, :])
            total = part if total is None else total + part
        slope = half + (0.5 * up) * (1.0 - tanh * tanh) * (GELU_C + (3.0 * GELU_A * GELU_C) * up2)
        d_act = dot_nt(dy, wdown_ref[cols, :]).astype(BF16).astype(F32)
        d_up = (d_act * slope).astype(BF16)
        dup_s[rows, cols] = d_up
        d_part = dot_nt(d_up, wup_ref[:, cols])
        dm = d_part if dm is None else dm + d_part
    if emit is not None:
        emit[rows, :] = (hid32 + total).astype(BF16)
    dm32 = dm.astype(BF16).astype(F32)
    lng_ref[2:3, :] += jnp.sum(dm32 * normed, axis=0, keepdims=True)
    lng_ref[3:4, :] += jnp.sum(dm32, axis=0, keepdims=True)
    d_hid32 = ln_back(dm32, normed, inv_std, ln_ref[2:3, :])
    d_hid = (d_hid32 + dy.astype(F32)).astype(BF16)
    dhid_s[rows, :] = d_hid
    datt_s[rows, :] = dot_nt(d_hid, wout_ref[...]).astype(BF16)


def mlp_grads(g_ref, m_s, act_s, dup_s, dhid_s, o_s, dy_ref):
    def chunk(c, _):
        cols = pl.ds(pl.multiple_of(c * D, D), D)
        g_ref[4 + c] = dot_tn(m_s[...], dup_s[:, cols])
        g_ref[8 + c] = dot_tn(act_s[:, cols], dy_ref[...])
        return 0
    lax.fori_loop(0, 4, chunk, 0)
    g_ref[3] = dot_tn(o_s[...], dhid_s[...])


def attn_backward(qkv_s, p_s, datt_s, dqkv_s):
    def heads(i, rows, pair):
        q2 = qkv_s[rows, pair_cols(0, pair)]
        k2 = qkv_s[rows, pair_cols(1, pair)]
        v2 = qkv_s[rows, pair_cols(2, pair)]
        do2 = datt_s[rows, pair_cols(0, pair)]
        dqs, dks, dvs = [], [], []
        for e in range(2):
            cut = slice(e * 64, e * 64 + 64)
            probs = p_s[i * 2 + e]
            d_out = do2[:, cut]
            d_probs = dot_nt(d_out, v2[:, cut]).astype(BF16).astype(F32)
            p32 = probs.astype(F32)
            row_dot = jnp.sum(d_probs * p32, axis=-1, keepdims=True)
            d_scores = (p32 * (d_probs - row_dot) * 0.125).astype(BF16)
            dqs.append(dot_nn(d_scores, k2[:, cut]).astype(BF16))
            dks.append(dot_tn(d_scores, q2[:, cut]).astype(BF16))
            dvs.append(dot_tn(probs, d_out).astype(BF16))
        dqkv_s[rows, pair_cols(0, pair)] = jnp.concatenate(dqs, axis=1)
        dqkv_s[rows, pair_cols(1, pair)] = jnp.concatenate(dks, axis=1)
        dqkv_s[rows, pair_cols(2, pair)] = jnp.concatenate(dvs, axis=1)
    head_pairs(heads)


def qkv_backward(x_ref, dqkv_s, dhid_s, ln_ref, wqkv_ref, a_s, dx_ref, lng_ref):
    def tile(rows):
        normed, inv_std = ln_norm(x_ref[rows, :].astype(F32))
        a_s[rows, :] = (normed * ln_ref[0:1, :] + ln_ref[1:2, :]).astype(BF16)
        da32 = dot_nt(dqkv_s[rows, :], wqkv_ref[...]).astype(BF16).astype(F32)
        lng_ref[0:1, :] += jnp.sum(da32 * normed, axis=0, keepdims=True)
        lng_ref[1:2, :] += jnp.sum(da32, axis=0, keepdims=True)
        d_in = ln_back(da32, normed, inv_std, ln_ref[0:1, :])
        dx_ref[rows, :] = (d_in + dhid_s[rows, :].astype(F32)).astype(BF16)
    row_tiles(tile)


def qkv_grads(g_ref, a_s, dqkv_s):
    def chunk(c, _):
        g_ref[c] = dot_tn(a_s[...], dqkv_s[:, pl.ds(pl.multiple_of(c * D, D), D)])
        return 0
    lax.fori_loop(0, 3, chunk, 0)


def spatial_forward_kernel(x_ref, ln_ref, wqkv_ref, wout_ref, wup_ref, wdown_ref, mid_ref, qkv_s, p_s, o_s, h_s):
    attn_forward(x_ref, ln_ref, wqkv_ref, qkv_s, p_s, o_s)

    def tail(rows):
        hid32 = hidden(x_ref, o_s, wout_ref, h_s, rows)
        mid_ref[rows, :] = mlp_forward(hid32, ln_ref, wup_ref, wdown_ref)
    row_tiles(tail)


def temporal_kernel(x_ref, dy_ref, ln_ref, wqkv_ref, wout_ref, wup_ref, wdown_ref, out_ref, dx_ref, g_ref, lng_ref,
                    qkv_s, p_s, o_s, h_s, m_s, act_s, dup_s, dhid_s, datt_s, dqkv_s, a_s):
    lng_ref[...] = jnp.zeros_like(lng_ref)
    attn_forward(x_ref, ln_ref, wqkv_ref, qkv_s, p_s, o_s)

    def tail(rows):
        hid32 = hidden(x_ref, o_s, wout_ref, h_s, rows)
        mlp_backward(hid32, dy_ref[rows, :], ln_ref, wup_ref, wout_ref, wdown_ref, m_s, act_s, dup_s, dhid_s, datt_s,
                     lng_ref, rows, out_ref)
    row_tiles(tail)
    attn_backward(qkv_s, p_s, datt_s, dqkv_s)
    qkv_backward(x_ref, dqkv_s, dhid_s, ln_ref, wqkv_ref, a_s, dx_ref, lng_ref)
    mlp_grads(g_ref, m_s, act_s, dup_s, dhid_s, o_s, dy_ref)
    qkv_grads(g_ref, a_s, dqkv_s)


def spatial_backward_kernel(x_ref, dy_ref, qkv_s, p_s, o_s, h_s, ln_ref, wqkv_ref, wout_ref, wup_ref, wdown_ref,
                            dx_ref, g_ref, lng_ref, m_s, act_s, dup_s, dhid_s, datt_s, dqkv_s, a_s):
    lng_ref[...] = jnp.zeros_like(lng_ref)

    def tail(rows):
        mlp_backward(h_s[rows, :].astype(F32), dy_ref[rows, :], ln_ref, wup_ref, wout_ref, wdown_ref, m_s, act_s, dup_s,
                     dhid_s, datt_s, lng_ref, rows, None)
    row_tiles(tail)
    mlp_grads(g_ref, m_s, act_s, dup_s, dhid_s, o_s, dy_ref)
    attn_backward(qkv_s, p_s, datt_s, dqkv_s)
    qkv_backward(x_ref, dqkv_s, dhid_s, ln_ref, wqkv_ref, a_s, dx_ref, lng_ref)
    qkv_grads(g_ref, a_s, dqkv_s)


def vmem_spec():
    return pl.BlockSpec(memory_space=pltpu.VMEM)


def call_kernel(kernel, args, outs, scratch, flops):
    return pl.pallas_call(
        kernel,
        out_shape=[jax.ShapeDtypeStruct(s, t) for s, t in outs],
        in_specs=[vmem_spec()] * len(args),
        out_specs=[vmem_spec()] * len(outs),
        scratch_shapes=[pltpu.VMEM(s, t) for s, t in scratch],
        compiler_params=pltpu.CompilerParams(vmem_limit_bytes=VMEM_LIMIT),
        cost_estimate=pl.CostEstimate(flops=flops, bytes_accessed=10_000_000, transcendentals=0),
    )(*args)


ACT = ((T, D), BF16)
QKV = ((T, 3 * D), BF16)
PROBS = ((12, SEQ, SEQ), BF16)
WIDE = ((T, FF), BF16)
GRAD = ((12, D, D), F32)
LNG = ((8, D), F32)
BACK_SCRATCH = [ACT, WIDE, WIDE, ACT, ACT, QKV, ACT]


def swap_kernel(n, src_ref, dst_ref, send_sem, recv_sem, local_sem):
    me = lax.axis_index("sp")
    mine = pltpu.make_async_copy(src_ref.at[me], dst_ref.at[me], local_sem)
    mine.start()

    def remote(k):
        to = lax.rem(me + k, n)
        return pltpu.make_async_remote_copy(src_ref.at[to], dst_ref.at[me], send_sem, recv_sem,
                                            device_id={"sp": to}, device_id_type=MESH)

    def start(k, _):
        remote(k).start()
        return 0
    lax.fori_loop(1, n, start, 0)
    mine.wait()
    whole = pltpu.make_async_copy(src_ref.at[pl.ds(0, n - 1)], dst_ref.at[pl.ds(0, n - 1)], send_sem)
    whole.wait()
    whole = pltpu.make_async_copy(src_ref.at[pl.ds(0, n - 1)], dst_ref.at[pl.ds(0, n - 1)], recv_sem)
    whole.wait()


def swap(n, pieces):
    return pl.pallas_call(
        functools.partial(swap_kernel, n),
        out_shape=jax.ShapeDtypeStruct(pieces.shape, pieces.dtype),
        in_specs=[vmem_spec()],
        out_specs=vmem_spec(),
        scratch_shapes=[pltpu.SemaphoreType.DMA] * 3,
        compiler_params=pltpu.CompilerParams(has_side_effects=True),
    )(pieces)


SIZES = (192, 96, 48, 24, 24, 24)
RECV_OFF = (0, 192, 288, 336, 360, 384)
RECV_ROWS = 408


def dim_info(me, dim):
    axis, far = dim // 2, dim % 2
    stride = (2, 8, 32)[axis]
    coord = lax.rem(lax.div(me, stride), 4)
    if far:
        bit = lax.div(coord, 2)
        partner = me + (3 - 2 * coord) * stride
    else:
        bit = lax.rem(coord + lax.div(coord, 2), 2)
        partner = me + (1 - 2 * lax.rem(coord, 2)) * stride
    return bit, partner


def reduce_kernel(g0_ref, g1_ref, ln_ref, o0_ref, o1_ref, oln_ref, acc, half, recv, lnacc, lnrecv,
                  half_send, half_recv, load_sem, send_sem, recv_sem, back_send, back_recv, out_send, out_recv, out_local,
                  ln_send, ln_recv, free_sem):
    me = lax.axis_index("sp")
    core = lax.rem(me, 2)
    sibling = me + 1 - 2 * core
    grads = (g0_ref, g1_ref)
    outs = (o0_ref, o1_ref)
    dims = [dim_info(me, d) for d in range(6)]

    def remote(src, dst, s_sem, r_sem, to):
        return pltpu.make_async_remote_copy(src, dst, s_sem, r_sem, device_id={"sp": to}, device_id_type=MESH)

    halves = {}
    loads = {}
    for p in range(6):
        for b in range(2):
            halves[b, p] = remote(grads[b].at[6 * (1 - core) + p], half.at[b, p], half_send.at[b, p], half_recv.at[b, p], sibling)
            halves[b, p].start()
            loads[b, p] = pltpu.make_async_copy(grads[b].at[6 * core + p], acc.at[b, p], load_sem.at[b, p])
            loads[b, p].start()

    lnacc[...] = ln_ref[...]
    ln_copies = []

    def ln_start(t):
        to = sibling if t == 0 else dims[t - 1][1]
        copy = remote(lnacc, lnrecv.at[t], ln_send.at[t], ln_recv.at[t], to)
        copy.start()
        ln_copies.append(copy)

    def ln_finish(t):
        ln_copies[t].wait()
        lnacc[...] += lnrecv[t]

    ln_start(0)

    offs = {}
    sends = {}

    def start_send(t, p, b):
        dim = (p + t) % 6
        bit, partner = dims[dim]
        off = offs[p, t]
        size = SIZES[t]
        if t < 4:
            keep = off + bit * size
            give = off + (1 - bit) * size
        else:
            keep = give = off
        offs[p, t + 1] = keep
        copy = remote(acc.at[b, p, pl.ds(pl.multiple_of(give, 8), size)], recv.at[b, p, pl.ds(RECV_OFF[t], size)],
                      send_sem.at[t, b, p], recv_sem.at[t, b, p], partner)
        copy.start()
        sends[t, p, b] = copy

    for p in range(6):
        offs[p, 0] = jnp.int32(0)
        for b in range(2):
            halves[b, p].wait()
            loads[b, p].wait()
            acc[b, p] += half[b, p]
            start_send(0, p, b)
    ln_finish(0)
    ln_start(1)
    backs = {}
    finals = []

    def forward(b, p, off, size, slot):
        rows = pl.ds(pl.multiple_of(off, 8), size)
        copy = remote(acc.at[b, p, rows], outs[b].at[6 * core + p, rows], out_send.at[slot, b, p], out_recv.at[slot, b, p], sibling)
        copy.start()
        finals.append(copy)
        copy = pltpu.make_async_copy(acc.at[b, p, rows], outs[b].at[6 * core + p, rows], out_local.at[slot, b, p])
        copy.start()
        finals.append(copy)

    def start_back(t, p, b):
        dim = (p + t) % 6
        _, partner = dims[dim]
        pl.semaphore_wait(free_sem.at[t, b, p], 1)
        rows = pl.ds(pl.multiple_of(offs[p, t + 1], 8), SIZES[t])
        copy = remote(acc.at[b, p, rows], acc.at[b, p, rows], back_send.at[t, b, p], back_recv.at[t, b, p], partner)
        copy.start()
        backs[t, p, b] = copy

    for t in range(6):
        for p in range(6):
            for b in range(2):
                sends[t, p, b].wait()
                if t < 4:
                    pl.semaphore_signal(free_sem.at[t, b, p], inc=1, device_id={"sp": dims[(p + t) % 6][1]}, device_id_type=MESH)
                size = SIZES[t]
                rows = pl.ds(pl.multiple_of(offs[p, t + 1], 8), size)
                acc[b, p, rows] += recv[b, p, pl.ds(RECV_OFF[t], size)]
                if t < 5:
                    start_send(t + 1, p, b)
                else:
                    start_back(3, p, b)
                    forward(b, p, offs[p, 4], 24, 0)
        ln_finish(t + 1)
        if t < 5:
            ln_start(t + 2)
    oln_ref[...] = lnacc[...]
    for t in (3, 2, 1, 0):
        for p in range(6):
            for b in range(2):
                backs[t, p, b].wait()
                if t > 0:
                    start_back(t - 1, p, b)
                bit = dims[(p + t) % 6][0]
                size = SIZES[t]
                forward(b, p, offs[p, t + 1] + (1 - 2 * bit) * size, size, 4 - t)
    for copy in finals:
        copy.wait()


def reduce_grads(g0, g1, ln):
    dma = pltpu.SemaphoreType.DMA
    any_spec = pl.BlockSpec(memory_space=pl.ANY)
    return pl.pallas_call(
        reduce_kernel,
        out_shape=[jax.ShapeDtypeStruct(g0.shape, F32), jax.ShapeDtypeStruct(g1.shape, F32), jax.ShapeDtypeStruct(ln.shape, F32)],
        in_specs=[any_spec, any_spec, vmem_spec()],
        out_specs=[any_spec, any_spec, vmem_spec()],
        scratch_shapes=[
            pltpu.VMEM((2, 6, D, D), F32), pltpu.VMEM((2, 6, D, D), F32), pltpu.VMEM((2, 6, RECV_ROWS, D), F32),
            pltpu.VMEM(ln.shape, F32), pltpu.VMEM((7,) + ln.shape, F32),
            dma((2, 6)), dma((2, 6)), dma((2, 6)), dma((6, 2, 6)), dma((6, 2, 6)), dma((4, 2, 6)), dma((4, 2, 6)),
            dma((5, 2, 6)), dma((5, 2, 6)), dma((5, 2, 6)), dma((7,)), dma((7,)),
            pltpu.SemaphoreType.REGULAR((4, 2, 6)),
        ],
        compiler_params=pltpu.CompilerParams(has_side_effects=True, vmem_limit_bytes=VMEM_LIMIT),
    )(g0, g1, ln)


def to_pieces(act, n):
    return act.reshape(2, n, 2, D).transpose(1, 0, 2, 3).reshape(n, 4, D)


def from_pieces(pieces, n):
    return pieces.reshape(n, 2, 2, D).transpose(2, 0, 1, 3).reshape(T, D)


def device_step(n, latents, cotangent, ln_params, w_qkv, w_out, w_up, w_down):
    ln32 = ln_params.astype(F32)
    weights = [(ln32[i], w_qkv[i], w_out[i].reshape(D, D), w_up[i], w_down[i]) for i in range(2)]
    x = latents.reshape(T, D)
    cot = from_pieces(swap(n, to_pieces(cotangent.reshape(T, D), n)), n)
    mid, qkv, probs, attn, hid = call_kernel(spatial_forward_kernel, (x,) + weights[0], [ACT, QKV, PROBS, ACT, ACT], [], 2_000_000_000)
    mid_t = from_pieces(swap(n, to_pieces(mid, n)), n)
    out, d_mid_t, g1, lng1 = call_kernel(temporal_kernel, (mid_t, cot) + weights[1], [ACT, ACT, GRAD, LNG],
                                         [QKV, PROBS, ACT, ACT] + BACK_SCRATCH, 6_000_000_000)
    d_mid = from_pieces(swap(n, to_pieces(d_mid_t, n)), n)
    result = from_pieces(swap(n, to_pieces(out, n)), n)
    dx, g0, lng0 = call_kernel(spatial_backward_kernel, (x, d_mid, qkv, probs, attn, hid) + weights[0], [ACT, GRAD, LNG],
                               BACK_SCRATCH, 4_000_000_000)
    r0, r1, rln = reduce_grads(g0, g1, jnp.concatenate([lng0, lng1], axis=0))
    blocks = jnp.stack([r0, r1])

    def wide(first, count):
        return blocks[:, first:first + count].transpose(0, 2, 1, 3).reshape(2, D, count * D)
    ln_grad = rln.reshape(2, 8, D)[:, :4]
    return (result.reshape(latents.shape), dx.reshape(latents.shape), ln_grad, wide(0, 3), blocks[:, 3].reshape(2, 6, 64, D),
            wide(4, 4), blocks[:, 8:12].reshape(2, FF, D))


def solution(mesh):
    act_spec = P('data', 'sp', None, None)
    replicated = P()
    part_spec = P('data')
    return jax.shard_map(functools.partial(device_step, mesh.shape["sp"]), mesh=mesh,
                         in_specs=(act_spec, act_spec, replicated, replicated, replicated, replicated, replicated),
                         out_specs=(act_spec, act_spec, part_spec, part_spec, part_spec, part_spec, part_spec),
                         check_vma=False)
```

```python
import functools

import jax
import jax.numpy as jnp
from jax import lax
from jax.experimental import pallas as pl
from jax.experimental.pallas import tpu as pltpu
from jax.sharding import PartitionSpec as P

F32 = jnp.float32
BF16 = jnp.bfloat16
D = 384
T = 512
SEQ = 256
FF = 1536
ROWS = 128
MESH = pl.DeviceIdType.MESH
VMEM_LIMIT = 60 * 1024 * 1024
GELU_C = 0.7978845608028654
GELU_A = 0.044715


def dot_nn(a, b):
    return lax.dot_general(a, b, (((1,), (0,)), ((), ())), preferred_element_type=F32)


def dot_nt(a, b):
    return lax.dot_general(a, b, (((1,), (1,)), ((), ())), preferred_element_type=F32)


def dot_tn(a, b):
    return lax.dot_general(a, b, (((0,), (0,)), ((), ())), preferred_element_type=F32)


def row_tiles(body, first=0, last=T // ROWS):
    def step(i, _):
        body(pl.ds(pl.multiple_of(i * ROWS, ROWS), ROWS))
        return 0
    lax.fori_loop(first, last, step, 0)


def ln_norm(x32):
    mean = jnp.sum(x32, axis=-1, keepdims=True) * (1.0 / D)
    centered = x32 - mean
    inv_std = lax.rsqrt(jnp.sum(centered * centered, axis=-1, keepdims=True) * (1.0 / D) + 1e-6)
    return centered * inv_std, inv_std


def ln_back(d32, normed, inv_std, gain):
    d_norm = d32 * gain
    d_center = d_norm - jnp.sum(d_norm, axis=-1, keepdims=True) * (1.0 / D)
    return inv_std * (d_center - normed * (jnp.sum(d_norm * normed, axis=-1, keepdims=True) * (1.0 / D)))


def head_pairs(body, first=0, last=6):
    def step(i, _):
        seq = i // 3
        pair = i - seq * 3
        rows = pl.ds(pl.multiple_of(seq * SEQ, SEQ), SEQ)
        body(i, rows, pair)
        return 0
    lax.fori_loop(first, last, step, 0)


def pair_cols(which, pair):
    return pl.ds(pl.multiple_of(which * D + pair * 128, 128), 128)


def attn_forward(x_ref, ln_ref, wqkv_ref, qkv_s, p_s, o_s):
    def qkv_tile(rows):
        normed, _ = ln_norm(x_ref[rows, :].astype(F32))
        a_in = (normed * ln_ref[0:1, :] + ln_ref[1:2, :]).astype(BF16)
        qkv_s[rows, :] = dot_nn(a_in, wqkv_ref[...]).astype(BF16)
    row_tiles(qkv_tile)

    def heads(i, rows, pair):
        q2 = qkv_s[rows, pair_cols(0, pair)]
        k2 = qkv_s[rows, pair_cols(1, pair)]
        v2 = qkv_s[rows, pair_cols(2, pair)]
        outs = []
        for e in range(2):
            cut = slice(e * 64, e * 64 + 64)
            scores = dot_nt(q2[:, cut], k2[:, cut]) * 0.125
            top = jnp.max(scores, axis=-1, keepdims=True)
            expd = jnp.exp(scores - top)
            total = jnp.sum(expd, axis=-1, keepdims=True)
            probs = (expd * (1.0 / total)).astype(BF16)
            p_s[i * 2 + e] = probs
            outs.append(dot_nn(probs, v2[:, cut]).astype(BF16))
        o_s[rows, pair_cols(0, pair)] = jnp.concatenate(outs, axis=1)
    head_pairs(heads)


def hidden(x_ref, o_s, wout_ref, h_s, rows):
    hid = (x_ref[rows, :].astype(F32) + dot_nn(o_s[rows, :], wout_ref[...])).astype(BF16)
    h_s[rows, :] = hid
    return hid.astype(F32)


def gelu_parts(up):
    up2 = up * up
    tanh = jnp.tanh(GELU_C * up * (1.0 + GELU_A * up2))
    half = 0.5 + 0.5 * tanh
    return up2, tanh, half


def mlp_forward(hid32, ln_ref, wup_ref, wdown_ref):
    normed, _ = ln_norm(hid32)
    m_in = (normed * ln_ref[2:3, :] + ln_ref[3:4, :]).astype(BF16)
    total = None
    for c in range(4):
        up = dot_nn(m_in, wup_ref[:, c * D:(c + 1) * D])
        act = (up * gelu_parts(up)[2]).astype(BF16)
        part = dot_nn(act, wdown_ref[c * D:(c + 1) * D, :])
        total = part if total is None else total + part
    return (hid32 + total).astype(BF16)


def mlp_backward(hid32, dy, ln_ref, wup_ref, wout_ref, wdown_ref, m_s, act_s, dup_s, dhid_s, datt_s, lng_ref, rows, emit):
    normed, inv_std = ln_norm(hid32)
    m_in = (normed * ln_ref[2:3, :] + ln_ref[3:4, :]).astype(BF16)
    m_s[rows, :] = m_in
    total = None
    dm = None
    for c in range(4):
        cols = slice(c * D, (c + 1) * D)
        up = dot_nn(m_in, wup_ref[:, cols])
        up2, tanh, half = gelu_parts(up)
        act = (up * half).astype(BF16)
        act_s[rows, cols] = act
        if emit is not None:
            part = dot_nn(act, wdown_ref[cols, :])
            total = part if total is None else total + part
        slope = half + (0.5 * up) * (1.0 - tanh * tanh) * (GELU_C + (3.0 * GELU_A * GELU_C) * up2)
        d_act = dot_nt(dy, wdown_ref[cols, :]).astype(BF16).astype(F32)
        d_up = (d_act * slope).astype(BF16)
        dup_s[rows, cols] = d_up
        d_part = dot_nt(d_up, wup_ref[:, cols])
        dm = d_part if dm is None else dm + d_part
    if emit is not None:
        emit[rows, :] = (hid32 + total).astype(BF16)
    dm32 = dm.astype(BF16).astype(F32)
    lng_ref[2:3, :] += jnp.sum(dm32 * normed, axis=0, keepdims=True)
    lng_ref[3:4, :] += jnp.sum(dm32, axis=0, keepdims=True)
    d_hid32 = ln_back(dm32, normed, inv_std, ln_ref[2:3, :])
    d_hid = (d_hid32 + dy.astype(F32)).astype(BF16)
    dhid_s[rows, :] = d_hid
    datt_s[rows, :] = dot_nt(d_hid, wout_ref[...]).astype(BF16)


def mlp_grads(g_ref, m_s, act_s, dup_s, dhid_s, o_s, dy_ref):
    def chunk(c, _):
        cols = pl.ds(pl.multiple_of(c * D, D), D)
        g_ref[4 + c] = dot_tn(m_s[...], dup_s[:, cols])
        g_ref[8 + c] = dot_tn(act_s[:, cols], dy_ref[...])
        return 0
    lax.fori_loop(0, 4, chunk, 0)
    g_ref[3] = dot_tn(o_s[...], dhid_s[...])


def attn_backward(qkv_s, p_s, datt_s, dqkv_s, first=0, last=6):
    def heads(i, rows, pair):
        q2 = qkv_s[rows, pair_cols(0, pair)]
        k2 = qkv_s[rows, pair_cols(1, pair)]
        v2 = qkv_s[rows, pair_cols(2, pair)]
        do2 = datt_s[rows, pair_cols(0, pair)]
        dqs, dks, dvs = [], [], []
        for e in range(2):
            cut = slice(e * 64, e * 64 + 64)
            probs = p_s[i * 2 + e]
            d_out = do2[:, cut]
            d_probs = dot_nt(d_out, v2[:, cut]).astype(BF16).astype(F32)
            p32 = probs.astype(F32)
            row_dot = jnp.sum(d_probs * p32, axis=-1, keepdims=True)
            d_scores = (p32 * (d_probs - row_dot) * 0.125).astype(BF16)
            dqs.append(dot_nn(d_scores, k2[:, cut]).astype(BF16))
            dks.append(dot_tn(d_scores, q2[:, cut]).astype(BF16))
            dvs.append(dot_tn(probs, d_out).astype(BF16))
        dqkv_s[rows, pair_cols(0, pair)] = jnp.concatenate(dqs, axis=1)
        dqkv_s[rows, pair_cols(1, pair)] = jnp.concatenate(dks, axis=1)
        dqkv_s[rows, pair_cols(2, pair)] = jnp.concatenate(dvs, axis=1)
    head_pairs(heads, first, last)


def qkv_backward(x_ref, dqkv_s, dhid_s, ln_ref, wqkv_ref, a_s, dx_ref, lng_ref):
    def tile(rows):
        normed, inv_std = ln_norm(x_ref[rows, :].astype(F32))
        a_s[rows, :] = (normed * ln_ref[0:1, :] + ln_ref[1:2, :]).astype(BF16)
        da32 = dot_nt(dqkv_s[rows, :], wqkv_ref[...]).astype(BF16).astype(F32)
        lng_ref[0:1, :] += jnp.sum(da32 * normed, axis=0, keepdims=True)
        lng_ref[1:2, :] += jnp.sum(da32, axis=0, keepdims=True)
        d_in = ln_back(da32, normed, inv_std, ln_ref[0:1, :])
        dx_ref[rows, :] = (d_in + dhid_s[rows, :].astype(F32)).astype(BF16)
    row_tiles(tile)


def qkv_grads(g_ref, a_s, dqkv_s):
    def chunk(c, _):
        g_ref[c] = dot_tn(a_s[...], dqkv_s[:, pl.ds(pl.multiple_of(c * D, D), D)])
        return 0
    lax.fori_loop(0, 3, chunk, 0)


def to_pieces(act_s, snd_ref):
    for a in range(2):
        snd_ref[:, a] = act_s[a * SEQ:(a + 1) * SEQ, :].reshape(SEQ // 2, 2, D)


def from_pieces(rcv_ref, dst_ref):
    flat = rcv_ref[...].reshape(T, D)
    row = lax.broadcasted_iota(jnp.int32, (SEQ, T), 0)
    col = lax.broadcasted_iota(jnp.int32, (SEQ, T), 1)
    for b in range(2):
        pick = (col == 2 * row + b).astype(F32).astype(BF16)
        dst_ref[b * SEQ:(b + 1) * SEQ, :] = dot_nn(pick, flat).astype(BF16)


HALF = D // 2
SIZES = (96, 48, 24, 24, 24, 24)
RECV_OFF = (0, 96, 144, 168, 192, 216)
RECV_ROWS = 240
HALVINGS = 3
ROUND_BLOCKS = ((4, 5, 6, 7, 8, 9), (10, 11, 3, 0, 1, 2))


def dim_info(me, dim):
    axis, far = dim // 2, dim % 2
    stride = (2, 8, 32)[axis]
    coord = lax.rem(lax.div(me, stride), 4)
    if far:
        bit = lax.div(coord, 2)
        partner = me + (3 - 2 * coord) * stride
    else:
        bit = lax.rem(coord + lax.div(coord, 2), 2)
        partner = me + (1 - 2 * lax.rem(coord, 2)) * stride
    return bit, partner


def remote_copy(src, dst, s_sem, r_sem, to):
    return pltpu.make_async_remote_copy(src, dst, s_sem, r_sem, device_id={"sp": to}, device_id_type=MESH)


def rows_at(start, size):
    return pl.ds(pl.multiple_of(start, 8), size)


class Round:
    def __init__(self, index, grads, blocks, out_refs, me, dims, half, recv, sems):
        self.r = index
        self.g = grads
        self.blocks = blocks
        self.out_refs = out_refs
        self.core = lax.rem(me, 2)
        self.sibling = me + 1 - 2 * self.core
        self.dims = dims
        self.half = half
        self.recv = recv
        (self.half_send, self.half_recv, self.send_sem, self.recv_sem, self.back_send, self.back_recv,
         self.fwd_send, self.fwd_recv, self.out_sem, self.free_sem, self.core_free) = sems
        self.offs = {(p, 0): self.core * HALF for p in range(6)}
        self.copies = {}
        self.forwards = {p: [] for p in range(6)}
        self.outs = []

    def start_core(self, parts=range(6)):
        for p in parts:
            copy = remote_copy(self.g.at[self.blocks[p], rows_at((1 - self.core) * HALF, HALF)], self.half.at[self.r, p],
                               self.half_send.at[self.r, p], self.half_recv.at[self.r, p], self.sibling)
            copy.start()
            self.copies["core", p] = copy

    def join_core(self):
        for p in range(6):
            self.copies["core", p].wait()
            pl.semaphore_signal(self.core_free.at[self.r, p], inc=1, device_id={"sp": self.sibling}, device_id_type=MESH)
            self.g[self.blocks[p], rows_at(self.core * HALF, HALF)] += self.half[self.r, p]
            self.start_send(0, p)

    def start_send(self, t, p):
        bit, partner = self.dims[(p + t) % 6]
        off, size = self.offs[p, t], SIZES[t]
        keep, give = (off + bit * size, off + (1 - bit) * size) if t < HALVINGS else (off, off)
        self.offs[p, t + 1] = keep
        copy = remote_copy(self.g.at[self.blocks[p], rows_at(give, size)], self.recv.at[self.r, p, pl.ds(RECV_OFF[t], size)],
                           self.send_sem.at[self.r, t, p], self.recv_sem.at[self.r, t, p], partner)
        copy.start()
        self.copies["send", t, p] = copy

    def step(self, t):
        size = SIZES[t]
        for p in range(6):
            self.copies["send", t, p].wait()
            if t < HALVINGS:
                pl.semaphore_signal(self.free_sem.at[self.r, t, p], inc=1, device_id={"sp": self.dims[(p + t) % 6][1]},
                                    device_id_type=MESH)
            self.g[self.blocks[p], rows_at(self.offs[p, t + 1], size)] += self.recv[self.r, p, pl.ds(RECV_OFF[t], size)]
            if t < 5:
                self.start_send(t + 1, p)
            else:
                self.start_back(HALVINGS - 1, p)
                pl.semaphore_wait(self.core_free.at[self.r, p], 1)
                self.forward(p, self.offs[p, HALVINGS], SIZES[HALVINGS - 1])

    def start_back(self, t, p):
        pl.semaphore_wait(self.free_sem.at[self.r, t, p], 1)
        rows = self.g.at[self.blocks[p], rows_at(self.offs[p, t + 1], SIZES[t])]
        copy = remote_copy(rows, rows, self.back_send.at[self.r, t, p], self.back_recv.at[self.r, t, p],
                           self.dims[(p + t) % 6][1])
        copy.start()
        self.copies["back", t, p] = copy

    def forward(self, p, off, size):
        rows = self.g.at[self.blocks[p], rows_at(off, size)]
        slot = len(self.forwards[p])
        copy = remote_copy(rows, rows, self.fwd_send.at[self.r, slot, p], self.fwd_recv.at[self.r, slot, p], self.sibling)
        copy.start()
        self.forwards[p].append(copy)

    def back(self, t):
        for p in range(6):
            self.copies["back", t, p].wait()
            if t > 0:
                self.start_back(t - 1, p)
            bit = self.dims[(p + t) % 6][0]
            self.forward(p, self.offs[p, t + 1] + (1 - 2 * bit) * SIZES[t], SIZES[t])

    def write(self):
        for p in range(6):
            for copy in self.forwards[p]:
                copy.wait()
            copy = pltpu.make_async_copy(self.g.at[self.blocks[p]], self.out_refs[self.blocks[p]], self.out_sem.at[self.r, p])
            copy.start()
            self.outs.append(copy)

    def finish(self):
        for copy in self.outs:
            copy.wait()


def out_slices(blk, gqkv, gout, gup, gdown):
    cols = [pl.ds(c * D, D) for c in range(4)]
    return ([gqkv.at[blk, :, cols[c]] for c in range(3)] + [gout.at[blk]] + [gup.at[blk, :, cols[c]] for c in range(4)]
            + [gdown.at[blk, cols[c]] for c in range(4)])


def step_kernel(n, x_hbm, cot_hbm, ln_in, wqkv_hbm, wout_hbm, wup_hbm, wdown_hbm,
                y_ref, dx_ref, gln_ref, gqkv, gout, gup, gdown,
                x_s, cot_s, mid_s, dmid_s, act_a, ln_s, wqkv, wout, wup, wdown, qkv_s, p_s, o_s, h_s,
                m_s, act_s, dup_s, dhid_s, datt_s, dqkv_s, a_s, snd, rcv, grads, half, recv, lnacc, lnrecv,
                load_sem, swap_send, swap_recv, swap_local, *sems):
    me = lax.axis_index("sp")
    dims = [dim_info(me, d) for d in range(6)]
    sibling = me + 1 - 2 * lax.rem(me, 2)
    ln_send, ln_recv = sems[-2:]
    sems = sems[:-2]

    barrier = pltpu.get_barrier_semaphore()

    def greet(k, _):
        pl.semaphore_signal(barrier, inc=1, device_id={"sp": lax.rem(me + k, n)}, device_id_type=MESH)
        return 0
    lax.fori_loop(1, n, greet, 0)

    loads = {}
    for name, src, dst in (("x", x_hbm, x_s), ("qkv0", wqkv_hbm.at[0], wqkv.at[0]), ("cot", cot_hbm, cot_s),
                           ("out0", wout_hbm.at[0], wout.at[0]), ("up0", wup_hbm.at[0], wup.at[0]),
                           ("down0", wdown_hbm.at[0], wdown.at[0]), ("qkv1", wqkv_hbm.at[1], wqkv.at[1]),
                           ("out1", wout_hbm.at[1], wout.at[1]), ("up1", wup_hbm.at[1], wup.at[1]),
                           ("down1", wdown_hbm.at[1], wdown.at[1])):
        loads[name] = pltpu.make_async_copy(src, dst, load_sem.at[len(loads)])
        loads[name].start()

    def need(*names):
        for name in names:
            loads[name].wait()

    def remote_piece(i, k):
        to = lax.rem(me + k, n)
        return remote_copy(snd.at[i, to], rcv.at[i, me], swap_send.at[i], swap_recv.at[i], to)

    def start_swap(i):
        pltpu.make_async_copy(snd.at[i, me], rcv.at[i, me], swap_local.at[i]).start()

        def send(k, _):
            remote_piece(i, k).start()
            return 0
        lax.fori_loop(1, n, send, 0)

    def end_swap(i):
        pltpu.make_async_copy(snd.at[i, me], rcv.at[i, me], swap_local.at[i]).wait()
        rest = pl.ds(0, n - 1)
        pltpu.make_async_copy(snd.at[i, rest], rcv.at[i, rest], swap_send.at[i]).wait()
        pltpu.make_async_copy(snd.at[i, rest], rcv.at[i, rest], swap_recv.at[i]).wait()

    ln_s[...] = ln_in[...].astype(F32)
    lnacc[...] = jnp.zeros_like(lnacc)
    ln = [ln_s.at[i] for i in range(2)]
    lng = [lnacc.at[pl.ds(8 * i, 8)] for i in range(2)]
    saved = [(qkv_s.at[i], p_s.at[i], o_s.at[i]) for i in range(2)]
    rounds = []
    for i in (1, 0):
        slices = out_slices(i, gqkv, gout, gup, gdown)
        for blocks in ROUND_BLOCKS:
            rounds.append(Round(len(rounds), grads.at[i], blocks, slices, me, dims, half, recv, sems))
    r1, r2, r3, r4 = rounds

    need("x", "qkv0")
    attn_forward(x_s, ln[0], wqkv.at[0], *saved[0])
    need("cot")
    to_pieces(cot_s, snd.at[0])
    pl.semaphore_wait(barrier, n - 1)
    start_swap(0)
    need("out0", "up0", "down0")

    def spatial_tail(rows):
        hid32 = hidden(x_s, o_s.at[0], wout.at[0], h_s.at[0], rows)
        mid_s[rows, :] = mlp_forward(hid32, ln[0], wup.at[0], wdown.at[0])
    row_tiles(spatial_tail)
    to_pieces(mid_s, snd.at[1])
    start_swap(1)

    need("qkv1", "out1", "up1", "down1")
    end_swap(0)
    from_pieces(rcv.at[0], cot_s)
    end_swap(1)
    from_pieces(rcv.at[1], mid_s)
    attn_forward(mid_s, ln[1], wqkv.at[1], *saved[1])

    def temporal_tail(rows):
        hid32 = hidden(mid_s, o_s.at[1], wout.at[1], h_s.at[1], rows)
        mlp_backward(hid32, cot_s[rows, :], ln[1], wup.at[1], wout.at[1], wdown.at[1], m_s, act_s, dup_s, dhid_s, datt_s,
                     lng[1], rows, act_a)
    row_tiles(temporal_tail)
    to_pieces(act_a, snd.at[2])
    start_swap(2)
    attn_backward(qkv_s.at[1], p_s.at[1], datt_s, dqkv_s)
    qkv_backward(mid_s, dqkv_s, dhid_s, ln[1], wqkv.at[1], a_s, dmid_s, lng[1])
    to_pieces(dmid_s, snd.at[3])
    start_swap(3)
    mlp_grads(grads.at[1], m_s, act_s, dup_s, dhid_s, o_s.at[1], cot_s)
    r1.start_core()
    qkv_grads(grads.at[1], a_s, dqkv_s)
    r2.start_core()
    end_swap(2)
    from_pieces(rcv.at[2], y_ref)
    r1.join_core()
    r2.join_core()
    end_swap(3)
    from_pieces(rcv.at[3], dmid_s)

    def back_tail(rows):
        mlp_backward(h_s[0, rows, :].astype(F32), dmid_s[rows, :], ln[0], wup.at[0], wout.at[0], wdown.at[0], m_s, act_s,
                     dup_s, dhid_s, datt_s, lng[0], rows, None)
    row_tiles(back_tail, 0, 2)
    r1.step(0)
    r2.step(0)
    row_tiles(back_tail, 2, 4)
    r1.step(1)
    r2.step(1)
    mlp_grads(grads.at[0], m_s, act_s, dup_s, dhid_s, o_s.at[0], dmid_s)
    r3.start_core()
    r1.step(2)
    r2.step(2)
    attn_backward(qkv_s.at[0], p_s.at[0], datt_s, dqkv_s, 0, 3)
    r1.step(3)
    r2.step(3)
    r3.join_core()
    attn_backward(qkv_s.at[0], p_s.at[0], datt_s, dqkv_s, 3, 6)
    r1.step(4)
    r2.step(4)
    r3.step(0)
    qkv_backward(x_s, dqkv_s, dhid_s, ln[0], wqkv.at[0], a_s, dx_ref, lng[0])
    r1.step(5)
    r2.step(5)
    r3.step(1)

    ln_copies = []

    def ln_start(t):
        to = sibling if t == 0 else dims[t - 1][1]
        copy = remote_copy(lnacc, lnrecv.at[t], ln_send.at[t], ln_recv.at[t], to)
        copy.start()
        ln_copies.append(copy)

    def ln_next():
        t = len(ln_copies) - 1
        ln_copies[t].wait()
        lnacc[...] += lnrecv[t]
        if t < 6:
            ln_start(t + 1)

    ln_start(0)
    qkv_grads(grads.at[0], a_s, dqkv_s)
    r4.start_core()
    r1.back(2)
    r2.back(2)
    r3.step(2)
    ln_next()
    r4.join_core()
    r1.back(1)
    r3.step(3)
    ln_next()
    r4.step(0)
    r2.back(1)
    r3.step(4)
    ln_next()
    r4.step(1)
    r1.back(0)
    r3.step(5)
    ln_next()
    r4.step(2)
    r2.back(0)
    r3.back(2)
    ln_next()
    r4.step(3)
    r3.back(1)
    ln_next()
    r4.step(4)
    r3.back(0)
    ln_next()
    r1.write()
    r2.write()
    r4.step(5)
    r4.back(2)
    r4.back(1)
    r3.write()
    r4.back(0)
    for i in range(2):
        gln_ref[i] = lnacc[8 * i:8 * i + 4, :]
    r4.write()
    for rnd in rounds:
        rnd.finish()


def device_step(n, latents, cotangent, ln_params, w_qkv, w_out, w_up, w_down):
    dma = pltpu.SemaphoreType.DMA
    regular = pltpu.SemaphoreType.REGULAR
    any_spec = pl.BlockSpec(memory_space=pl.ANY)
    vmem_spec = pl.BlockSpec(memory_space=pltpu.VMEM)
    act, wide, qkv = (T, D), (T, FF), (T, 3 * D)
    y, dx, gln, gqkv, gout, gup, gdown = pl.pallas_call(
        functools.partial(step_kernel, n),
        out_shape=[jax.ShapeDtypeStruct(act, BF16)] * 2 + [jax.ShapeDtypeStruct(s, F32) for s in (
            (2, 4, D), (2, D, 3 * D), (2, D, D), (2, D, FF), (2, FF, D))],
        in_specs=[any_spec, any_spec, vmem_spec] + [any_spec] * 4,
        out_specs=[vmem_spec] * 3 + [any_spec] * 4,
        scratch_shapes=[pltpu.VMEM(s, BF16) for s in [act] * 5]
        + [pltpu.VMEM((2, 4, D), F32)]
        + [pltpu.VMEM((2,) + s, BF16) for s in ((D, 3 * D), (D, D), (D, FF), (FF, D), qkv, (12, SEQ, SEQ), act, act)]
        + [pltpu.VMEM(s, BF16) for s in (act, wide, wide, act, act, qkv, act)]
        + [pltpu.VMEM((4, n, 2, 2, D), BF16)] * 2
        + [pltpu.VMEM((2, 12, D, D), F32), pltpu.VMEM((4, 6, HALF, D), F32), pltpu.VMEM((4, 6, RECV_ROWS, D), F32),
           pltpu.VMEM((16, D), F32), pltpu.VMEM((7, 16, D), F32)]
        + [dma((10,)), dma((4,)), dma((4,)), dma((4,))]
        + [dma((4, 6)), dma((4, 6)), dma((4, 6, 6)), dma((4, 6, 6)), dma((4, 3, 6)), dma((4, 3, 6)), dma((4, 4, 6)),
           dma((4, 4, 6)), dma((4, 6)), regular((4, 3, 6)), regular((4, 6)), dma((7,)), dma((7,))],
        compiler_params=pltpu.CompilerParams(collective_id=0, has_side_effects=True, vmem_limit_bytes=67_000_000),
        cost_estimate=pl.CostEstimate(flops=12_000_000_000, bytes_accessed=30_000_000, transcendentals=0),
    )(latents.reshape(T, D), cotangent.reshape(T, D), ln_params, w_qkv, w_out.reshape(2, D, D), w_up, w_down)
    return (y.reshape(latents.shape), dx.reshape(latents.shape), gln, gqkv, gout.reshape(2, 6, 64, D), gup, gdown)


def solution(mesh):
    act_spec = P('data', 'sp', None, None)
    replicated = P()
    part_spec = P('data')
    return jax.shard_map(functools.partial(device_step, mesh.shape["sp"]), mesh=mesh,
                         in_specs=(act_spec, act_spec, replicated, replicated, replicated, replicated, replicated),
                         out_specs=(act_spec, act_spec, part_spec, part_spec, part_spec, part_spec, part_spec),
                         check_vma=False)
```

```python
import functools

import jax
import jax.numpy as jnp
from jax import lax
from jax.experimental import pallas as pl
from jax.experimental.pallas import tpu as pltpu
from jax.sharding import PartitionSpec as P

F32 = jnp.float32
BF16 = jnp.bfloat16
D = 384
T = 512
SEQ = 256
FF = 1536
ROWS = 128
MESH = pl.DeviceIdType.MESH
STEP_VMEM = 48_000_000
GELU_C = 0.7978845608028654
GELU_A = 0.044715


def dot_nn(a, b):
    return lax.dot_general(a, b, (((1,), (0,)), ((), ())), preferred_element_type=F32)


def dot_nt(a, b):
    return lax.dot_general(a, b, (((1,), (1,)), ((), ())), preferred_element_type=F32)


def dot_tn(a, b):
    return lax.dot_general(a, b, (((0,), (0,)), ((), ())), preferred_element_type=F32)


def row_tiles(body, first=0, last=T // ROWS):
    def step(i, _):
        body(pl.ds(pl.multiple_of(i * ROWS, ROWS), ROWS))
        return 0
    lax.fori_loop(first, last, step, 0)


def ln_norm(x32):
    mean = jnp.sum(x32, axis=-1, keepdims=True) * (1.0 / D)
    centered = x32 - mean
    inv_std = lax.rsqrt(jnp.sum(centered * centered, axis=-1, keepdims=True) * (1.0 / D) + 1e-6)
    return centered * inv_std, inv_std


def ln_back(d32, normed, inv_std, gain):
    d_norm = d32 * gain
    d_center = d_norm - jnp.sum(d_norm, axis=-1, keepdims=True) * (1.0 / D)
    return inv_std * (d_center - normed * (jnp.sum(d_norm * normed, axis=-1, keepdims=True) * (1.0 / D)))


def head_pairs(body, first=0, last=6):
    def step(i, _):
        seq = i // 3
        pair = i - seq * 3
        rows = pl.ds(pl.multiple_of(seq * SEQ, SEQ), SEQ)
        body(i, rows, pair)
        return 0
    lax.fori_loop(first, last, step, 0)


def pair_cols(which, pair):
    return pl.ds(pl.multiple_of(which * D + pair * 128, 128), 128)


def attn_forward(x_ref, ln_ref, wqkv_ref, qkv_s, p_s, o_s):
    def qkv_tile(rows):
        normed, _ = ln_norm(x_ref[rows, :].astype(F32))
        a_in = (normed * ln_ref[0:1, :] + ln_ref[1:2, :]).astype(BF16)
        qkv_s[rows, :] = dot_nn(a_in, wqkv_ref[...]).astype(BF16)
    row_tiles(qkv_tile)

    def heads(i, rows, pair):
        q2 = qkv_s[rows, pair_cols(0, pair)]
        k2 = qkv_s[rows, pair_cols(1, pair)]
        v2 = qkv_s[rows, pair_cols(2, pair)]
        outs = []
        for e in range(2):
            cut = slice(e * 64, e * 64 + 64)
            scores = dot_nt(q2[:, cut], k2[:, cut]) * 0.125
            top = jnp.max(scores, axis=-1, keepdims=True)
            expd = jnp.exp(scores - top)
            total = jnp.sum(expd, axis=-1, keepdims=True)
            probs = (expd * (1.0 / total)).astype(BF16)
            p_s[i * 2 + e] = probs
            outs.append(dot_nn(probs, v2[:, cut]).astype(BF16))
        o_s[rows, pair_cols(0, pair)] = jnp.concatenate(outs, axis=1)
    head_pairs(heads)


def hidden(x_ref, o_s, wout_ref, h_s, rows):
    hid = (x_ref[rows, :].astype(F32) + dot_nn(o_s[rows, :], wout_ref[...])).astype(BF16)
    h_s[rows, :] = hid
    return hid.astype(F32)


def gelu_parts(up):
    up2 = up * up
    tanh = jnp.tanh(GELU_C * up * (1.0 + GELU_A * up2))
    half = 0.5 + 0.5 * tanh
    return up2, tanh, half


def mlp_forward(hid32, ln_ref, wup_ref, wdown_ref):
    normed, _ = ln_norm(hid32)
    m_in = (normed * ln_ref[2:3, :] + ln_ref[3:4, :]).astype(BF16)
    total = None
    for c in range(4):
        up = dot_nn(m_in, wup_ref[:, c * D:(c + 1) * D])
        act = (up * gelu_parts(up)[2]).astype(BF16)
        part = dot_nn(act, wdown_ref[c * D:(c + 1) * D, :])
        total = part if total is None else total + part
    return (hid32 + total).astype(BF16)


def mlp_backward(hid32, dy, ln_ref, wup_ref, wout_ref, wdown_ref, m_s, act_s, dup_s, dhid_s, datt_s, lng_ref, rows, emit):
    normed, inv_std = ln_norm(hid32)
    m_in = (normed * ln_ref[2:3, :] + ln_ref[3:4, :]).astype(BF16)
    m_s[rows, :] = m_in
    total = None
    dm = None
    for c in range(4):
        cols = slice(c * D, (c + 1) * D)
        up = dot_nn(m_in, wup_ref[:, cols])
        up2, tanh, half = gelu_parts(up)
        act = (up * half).astype(BF16)
        act_s[rows, cols] = act
        if emit is not None:
            part = dot_nn(act, wdown_ref[cols, :])
            total = part if total is None else total + part
        slope = half + (0.5 * up) * (1.0 - tanh * tanh) * (GELU_C + (3.0 * GELU_A * GELU_C) * up2)
        d_act = dot_nt(dy, wdown_ref[cols, :]).astype(BF16).astype(F32)
        d_up = (d_act * slope).astype(BF16)
        dup_s[rows, cols] = d_up
        d_part = dot_nt(d_up, wup_ref[:, cols])
        dm = d_part if dm is None else dm + d_part
    if emit is not None:
        emit[rows, :] = (hid32 + total).astype(BF16)
    dm32 = dm.astype(BF16).astype(F32)
    lng_ref[2:3, :] += jnp.sum(dm32 * normed, axis=0, keepdims=True)
    lng_ref[3:4, :] += jnp.sum(dm32, axis=0, keepdims=True)
    d_hid32 = ln_back(dm32, normed, inv_std, ln_ref[2:3, :])
    d_hid = (d_hid32 + dy.astype(F32)).astype(BF16)
    dhid_s[rows, :] = d_hid
    datt_s[rows, :] = dot_nt(d_hid, wout_ref[...]).astype(BF16)


def mlp_grads(g_ref, m_s, act_s, dup_s, dhid_s, o_s, dy_ref):
    def chunk(c, _):
        cols = pl.ds(pl.multiple_of(c * D, D), D)
        g_ref[4 + c] = dot_tn(m_s[...], dup_s[:, cols])
        g_ref[8 + c] = dot_tn(act_s[:, cols], dy_ref[...])
        return 0
    lax.fori_loop(0, 4, chunk, 0)
    g_ref[3] = dot_tn(o_s[...], dhid_s[...])


def attn_backward(qkv_s, p_s, datt_s, dqkv_s, first=0, last=6):
    def heads(i, rows, pair):
        q2 = qkv_s[rows, pair_cols(0, pair)]
        k2 = qkv_s[rows, pair_cols(1, pair)]
        v2 = qkv_s[rows, pair_cols(2, pair)]
        do2 = datt_s[rows, pair_cols(0, pair)]
        dqs, dks, dvs = [], [], []
        for e in range(2):
            cut = slice(e * 64, e * 64 + 64)
            probs = p_s[i * 2 + e]
            d_out = do2[:, cut]
            d_probs = dot_nt(d_out, v2[:, cut]).astype(BF16).astype(F32)
            p32 = probs.astype(F32)
            row_dot = jnp.sum(d_probs * p32, axis=-1, keepdims=True)
            d_scores = (p32 * (d_probs - row_dot) * 0.125).astype(BF16)
            dqs.append(dot_nn(d_scores, k2[:, cut]).astype(BF16))
            dks.append(dot_tn(d_scores, q2[:, cut]).astype(BF16))
            dvs.append(dot_tn(probs, d_out).astype(BF16))
        dqkv_s[rows, pair_cols(0, pair)] = jnp.concatenate(dqs, axis=1)
        dqkv_s[rows, pair_cols(1, pair)] = jnp.concatenate(dks, axis=1)
        dqkv_s[rows, pair_cols(2, pair)] = jnp.concatenate(dvs, axis=1)
    head_pairs(heads, first, last)


def qkv_backward(x_ref, dqkv_s, dhid_s, ln_ref, wqkv_ref, a_s, dx_ref, lng_ref):
    def tile(rows):
        normed, inv_std = ln_norm(x_ref[rows, :].astype(F32))
        a_s[rows, :] = (normed * ln_ref[0:1, :] + ln_ref[1:2, :]).astype(BF16)
        da32 = dot_nt(dqkv_s[rows, :], wqkv_ref[...]).astype(BF16).astype(F32)
        lng_ref[0:1, :] += jnp.sum(da32 * normed, axis=0, keepdims=True)
        lng_ref[1:2, :] += jnp.sum(da32, axis=0, keepdims=True)
        d_in = ln_back(da32, normed, inv_std, ln_ref[0:1, :])
        dx_ref[rows, :] = (d_in + dhid_s[rows, :].astype(F32)).astype(BF16)
    row_tiles(tile)


def qkv_grads(g_ref, a_s, dqkv_s):
    def chunk(c, _):
        g_ref[c] = dot_tn(a_s[...], dqkv_s[:, pl.ds(pl.multiple_of(c * D, D), D)])
        return 0
    lax.fori_loop(0, 3, chunk, 0)


def to_pieces(act_s, snd_ref):
    for a in range(2):
        snd_ref[:, a] = act_s[a * SEQ:(a + 1) * SEQ, :].reshape(SEQ // 2, 2, D)


def from_pieces(rcv_ref, dst_ref):
    flat = rcv_ref[...].reshape(T, D)
    row = lax.broadcasted_iota(jnp.int32, (SEQ, T), 0)
    col = lax.broadcasted_iota(jnp.int32, (SEQ, T), 1)
    for b in range(2):
        pick = (col == 2 * row + b).astype(F32).astype(BF16)
        dst_ref[b * SEQ:(b + 1) * SEQ, :] = dot_nn(pick, flat).astype(BF16)


HALF = D // 2
SIZES = (96, 48, 24, 24, 24, 24)
RECV_OFF = (0, 96, 144, 168, 192, 216)
RECV_ROWS = 240
HALVINGS = 3
ROUND_BLOCKS = ((4, 5, 6, 7, 8, 9), (10, 11, 3, 0, 1, 2))


def dim_info(me, dim):
    axis, far = dim // 2, dim % 2
    stride = (2, 8, 32)[axis]
    coord = lax.rem(lax.div(me, stride), 4)
    if far:
        bit = lax.div(coord, 2)
        partner = me + (3 - 2 * coord) * stride
    else:
        bit = lax.rem(coord + lax.div(coord, 2), 2)
        partner = me + (1 - 2 * lax.rem(coord, 2)) * stride
    return bit, partner


def remote_copy(src, dst, s_sem, r_sem, to):
    return pltpu.make_async_remote_copy(src, dst, s_sem, r_sem, device_id={"sp": to}, device_id_type=MESH)


def rows_at(start, size):
    return pl.ds(pl.multiple_of(start, 8), size)


class Round:
    def __init__(self, index, grads, blocks, me, dims, half, recv, sems):
        self.r = index
        self.g = grads
        self.blocks = blocks
        self.core = lax.rem(me, 2)
        self.sibling = me + 1 - 2 * self.core
        self.dims = dims
        self.half = half
        self.recv = recv
        (self.half_send, self.half_recv, self.send_sem, self.recv_sem, self.back_send, self.back_recv,
         self.fwd_send, self.fwd_recv, self.free_sem, self.core_free) = sems
        self.offs = {(p, 0): self.core * HALF for p in range(6)}
        self.copies = {}
        self.forwards = {p: [] for p in range(6)}

    def start_core(self, parts=range(6)):
        for p in parts:
            copy = remote_copy(self.g.at[self.blocks[p], rows_at((1 - self.core) * HALF, HALF)], self.half.at[self.r, p],
                               self.half_send.at[self.r, p], self.half_recv.at[self.r, p], self.sibling)
            copy.start()
            self.copies["core", p] = copy

    def join_core(self):
        for p in range(6):
            self.copies["core", p].wait()
            pl.semaphore_signal(self.core_free.at[self.r, p], inc=1, device_id={"sp": self.sibling}, device_id_type=MESH)
            self.g[self.blocks[p], rows_at(self.core * HALF, HALF)] += self.half[self.r, p]
            self.start_send(0, p)

    def start_send(self, t, p):
        bit, partner = self.dims[(p + t) % 6]
        off, size = self.offs[p, t], SIZES[t]
        keep, give = (off + bit * size, off + (1 - bit) * size) if t < HALVINGS else (off, off)
        self.offs[p, t + 1] = keep
        copy = remote_copy(self.g.at[self.blocks[p], rows_at(give, size)], self.recv.at[self.r, p, pl.ds(RECV_OFF[t], size)],
                           self.send_sem.at[self.r, t, p], self.recv_sem.at[self.r, t, p], partner)
        copy.start()
        self.copies["send", t, p] = copy

    def step(self, t):
        size = SIZES[t]
        for p in range(6):
            self.copies["send", t, p].wait()
            if t < HALVINGS:
                pl.semaphore_signal(self.free_sem.at[self.r, t, p], inc=1, device_id={"sp": self.dims[(p + t) % 6][1]},
                                    device_id_type=MESH)
            self.g[self.blocks[p], rows_at(self.offs[p, t + 1], size)] += self.recv[self.r, p, pl.ds(RECV_OFF[t], size)]
            if t < 5:
                self.start_send(t + 1, p)
            else:
                self.start_back(HALVINGS - 1, p)
                pl.semaphore_wait(self.core_free.at[self.r, p], 1)
                self.forward(p, self.offs[p, HALVINGS], SIZES[HALVINGS - 1])

    def start_back(self, t, p):
        pl.semaphore_wait(self.free_sem.at[self.r, t, p], 1)
        rows = self.g.at[self.blocks[p], rows_at(self.offs[p, t + 1], SIZES[t])]
        copy = remote_copy(rows, rows, self.back_send.at[self.r, t, p], self.back_recv.at[self.r, t, p],
                           self.dims[(p + t) % 6][1])
        copy.start()
        self.copies["back", t, p] = copy

    def forward(self, p, off, size):
        rows = self.g.at[self.blocks[p], rows_at(off, size)]
        slot = len(self.forwards[p])
        copy = remote_copy(rows, rows, self.fwd_send.at[self.r, slot, p], self.fwd_recv.at[self.r, slot, p], self.sibling)
        copy.start()
        self.forwards[p].append(copy)

    def back(self, t):
        for p in range(6):
            self.copies["back", t, p].wait()
            if t > 0:
                self.start_back(t - 1, p)
            bit = self.dims[(p + t) % 6][0]
            self.forward(p, self.offs[p, t + 1] + (1 - 2 * bit) * SIZES[t], SIZES[t])

    def finish(self):
        for p in range(6):
            for copy in self.forwards[p]:
                copy.wait()


def out_slices(blk, gqkv, gout, gup, gdown):
    cols = [pl.ds(c * D, D) for c in range(4)]
    return ([gqkv.at[blk, :, cols[c]] for c in range(3)] + [gout.at[blk]] + [gup.at[blk, :, cols[c]] for c in range(4)]
            + [gdown.at[blk, cols[c]] for c in range(4)])


def step_kernel(n, x_hbm, cot_hbm, ln_in, wqkv_hbm, wout_hbm, wup_hbm, wdown_hbm,
                y_ref, dx_ref, gln_ref, grads,
                x_s, cot_s, mid_s, dmid_s, act_a, ln_s, wqkv, wout, wup, wdown, qkv_s, p_s, o_s, h_s,
                m_s, act_s, dup_s, dhid_s, datt_s, dqkv_s, a_s, snd, rcv, half, recv, lnacc, lnrecv,
                load_sem, swap_send, swap_recv, swap_local, *sems):
    me = lax.axis_index("sp")
    dims = [dim_info(me, d) for d in range(6)]
    sibling = me + 1 - 2 * lax.rem(me, 2)
    ln_send, ln_recv = sems[-2:]
    sems = sems[:-2]

    barrier = pltpu.get_barrier_semaphore()

    def greet(k, _):
        pl.semaphore_signal(barrier, inc=1, device_id={"sp": lax.rem(me + k, n)}, device_id_type=MESH)
        return 0
    lax.fori_loop(1, n, greet, 0)

    loads = {}
    for name, src, dst in (("x", x_hbm, x_s), ("qkv0", wqkv_hbm.at[0], wqkv.at[0]), ("cot", cot_hbm, cot_s),
                           ("out0", wout_hbm.at[0], wout.at[0]), ("up0", wup_hbm.at[0], wup.at[0]),
                           ("down0", wdown_hbm.at[0], wdown.at[0]), ("qkv1", wqkv_hbm.at[1], wqkv.at[1]),
                           ("out1", wout_hbm.at[1], wout.at[1]), ("up1", wup_hbm.at[1], wup.at[1]),
                           ("down1", wdown_hbm.at[1], wdown.at[1])):
        loads[name] = pltpu.make_async_copy(src, dst, load_sem.at[len(loads)])
        loads[name].start()

    def need(*names):
        for name in names:
            loads[name].wait()

    def remote_piece(i, k):
        to = lax.rem(me + k, n)
        return remote_copy(snd.at[i, to], rcv.at[i, me], swap_send.at[i], swap_recv.at[i], to)

    def start_swap(i):
        pltpu.make_async_copy(snd.at[i, me], rcv.at[i, me], swap_local.at[i]).start()

        def send(k, _):
            remote_piece(i, k).start()
            return 0
        lax.fori_loop(1, n, send, 0)

    def end_swap(i):
        pltpu.make_async_copy(snd.at[i, me], rcv.at[i, me], swap_local.at[i]).wait()
        rest = pl.ds(0, n - 1)
        pltpu.make_async_copy(snd.at[i, rest], rcv.at[i, rest], swap_send.at[i]).wait()
        pltpu.make_async_copy(snd.at[i, rest], rcv.at[i, rest], swap_recv.at[i]).wait()

    ln_s[...] = ln_in[...].astype(F32)
    lnacc[...] = jnp.zeros_like(lnacc)
    ln = [ln_s.at[i] for i in range(2)]
    lng = [lnacc.at[pl.ds(8 * i, 8)] for i in range(2)]
    saved = [(qkv_s.at[i], p_s.at[i], o_s.at[i]) for i in range(2)]
    rounds = []
    for i in (1, 0):
        for blocks in ROUND_BLOCKS:
            rounds.append(Round(len(rounds), grads.at[i], blocks, me, dims, half, recv, sems))
    r1, r2, r3, r4 = rounds

    need("x", "qkv0")
    attn_forward(x_s, ln[0], wqkv.at[0], *saved[0])
    need("cot")
    to_pieces(cot_s, snd.at[0])
    need("out0", "up0", "down0")

    def spatial_tail(rows):
        hid32 = hidden(x_s, o_s.at[0], wout.at[0], h_s.at[0], rows)
        mid_s[rows, :] = mlp_forward(hid32, ln[0], wup.at[0], wdown.at[0])
    row_tiles(spatial_tail)
    to_pieces(mid_s, snd.at[1])
    pl.semaphore_wait(barrier, n - 1)
    start_swap(1)
    start_swap(0)

    need("qkv1", "out1", "up1", "down1")
    end_swap(1)
    from_pieces(rcv.at[1], mid_s)
    attn_forward(mid_s, ln[1], wqkv.at[1], *saved[1])
    end_swap(0)
    from_pieces(rcv.at[0], cot_s)

    def temporal_tail(rows):
        hid32 = hidden(mid_s, o_s.at[1], wout.at[1], h_s.at[1], rows)
        mlp_backward(hid32, cot_s[rows, :], ln[1], wup.at[1], wout.at[1], wdown.at[1], m_s, act_s, dup_s, dhid_s, datt_s,
                     lng[1], rows, act_a)
    row_tiles(temporal_tail)
    to_pieces(act_a, snd.at[2])
    start_swap(2)
    attn_backward(qkv_s.at[1], p_s.at[1], datt_s, dqkv_s)
    qkv_backward(mid_s, dqkv_s, dhid_s, ln[1], wqkv.at[1], a_s, dmid_s, lng[1])
    to_pieces(dmid_s, snd.at[3])
    start_swap(3)
    mlp_grads(grads.at[1], m_s, act_s, dup_s, dhid_s, o_s.at[1], cot_s)
    r1.start_core()
    qkv_grads(grads.at[1], a_s, dqkv_s)
    r2.start_core()
    end_swap(2)
    from_pieces(rcv.at[2], y_ref)
    r1.join_core()
    r2.join_core()
    end_swap(3)
    from_pieces(rcv.at[3], dmid_s)

    def back_tail(rows):
        mlp_backward(h_s[0, rows, :].astype(F32), dmid_s[rows, :], ln[0], wup.at[0], wout.at[0], wdown.at[0], m_s, act_s,
                     dup_s, dhid_s, datt_s, lng[0], rows, None)
    row_tiles(back_tail, 0, 2)
    r1.step(0)
    r2.step(0)
    row_tiles(back_tail, 2, 4)
    r1.step(1)
    r2.step(1)
    mlp_grads(grads.at[0], m_s, act_s, dup_s, dhid_s, o_s.at[0], dmid_s)
    r3.start_core()
    r1.step(2)
    r2.step(2)
    attn_backward(qkv_s.at[0], p_s.at[0], datt_s, dqkv_s, 0, 3)
    r1.step(3)
    r2.step(3)
    r3.join_core()
    attn_backward(qkv_s.at[0], p_s.at[0], datt_s, dqkv_s, 3, 6)
    r1.step(4)
    r2.step(4)
    r3.step(0)
    qkv_backward(x_s, dqkv_s, dhid_s, ln[0], wqkv.at[0], a_s, dx_ref, lng[0])
    r1.step(5)
    r2.step(5)
    r3.step(1)

    ln_copies = []

    def ln_start(t):
        to = sibling if t == 0 else dims[t - 1][1]
        copy = remote_copy(lnacc, lnrecv.at[t], ln_send.at[t], ln_recv.at[t], to)
        copy.start()
        ln_copies.append(copy)

    def ln_next():
        t = len(ln_copies) - 1
        ln_copies[t].wait()
        lnacc[...] += lnrecv[t]
        if t < 6:
            ln_start(t + 1)

    ln_start(0)
    qkv_grads(grads.at[0], a_s, dqkv_s)
    r4.start_core()
    r1.back(2)
    r2.back(2)
    r3.step(2)
    ln_next()
    r4.join_core()
    r1.back(1)
    r3.step(3)
    ln_next()
    r4.step(0)
    r2.back(1)
    r3.step(4)
    ln_next()
    r4.step(1)
    r1.back(0)
    r3.step(5)
    ln_next()
    r4.step(2)
    r2.back(0)
    r3.back(2)
    ln_next()
    r4.step(3)
    r3.back(1)
    ln_next()
    r4.step(4)
    r3.back(0)
    ln_next()
    r4.step(5)
    r4.back(2)
    r4.back(1)
    r4.back(0)
    for i in range(2):
        gln_ref[i] = lnacc[8 * i:8 * i + 4, :]
    for rnd in rounds:
        rnd.finish()


def publish_kernel(y_in, dx_in, gln_in, grads, y_ref, dx_ref, gln_ref, gqkv, gout, gup, gdown, sem):
    pairs = [(y_in, y_ref), (dx_in, dx_ref), (gln_in, gln_ref)]
    for i in range(2):
        slices = out_slices(i, gqkv, gout, gup, gdown)
        pairs += [(grads.at[i, j], slices[j]) for j in range(12)]
    copies = [pltpu.make_async_copy(src, dst, sem.at[k]) for k, (src, dst) in enumerate(pairs)]
    for copy in copies:
        copy.start()
    for copy in copies:
        copy.wait()


def device_step(n, latents, cotangent, ln_params, w_qkv, w_out, w_up, w_down):
    dma = pltpu.SemaphoreType.DMA
    regular = pltpu.SemaphoreType.REGULAR
    any_spec = pl.BlockSpec(memory_space=pl.ANY)
    vmem_spec = pl.BlockSpec(memory_space=pltpu.VMEM)
    act, wide, qkv = (T, D), (T, FF), (T, 3 * D)
    shapes = [(act, BF16), (act, BF16), ((2, 4, D), F32)]
    held = pl.pallas_call(
        functools.partial(step_kernel, n),
        out_shape=[pltpu.VMEM(s, t) for s, t in shapes] + [pltpu.VMEM((2, 12, D, D), F32)],
        in_specs=[any_spec, any_spec, vmem_spec] + [any_spec] * 4,
        out_specs=[vmem_spec] * 4,
        scratch_shapes=[pltpu.VMEM(s, BF16) for s in [act] * 5]
        + [pltpu.VMEM((2, 4, D), F32)]
        + [pltpu.VMEM((2,) + s, BF16) for s in ((D, 3 * D), (D, D), (D, FF), (FF, D), qkv, (12, SEQ, SEQ), act, act)]
        + [pltpu.VMEM(s, BF16) for s in (act, wide, wide, act, act, qkv, act)]
        + [pltpu.VMEM((4, n, 2, 2, D), BF16)] * 2
        + [pltpu.VMEM((4, 6, HALF, D), F32), pltpu.VMEM((4, 6, RECV_ROWS, D), F32),
           pltpu.VMEM((16, D), F32), pltpu.VMEM((7, 16, D), F32)]
        + [dma((10,)), dma((4,)), dma((4,)), dma((4,))]
        + [dma((4, 6)), dma((4, 6)), dma((4, 6, 6)), dma((4, 6, 6)), dma((4, 3, 6)), dma((4, 3, 6)), dma((4, 4, 6)),
           dma((4, 4, 6)), regular((4, 3, 6)), regular((4, 6)), dma((7,)), dma((7,))],
        compiler_params=pltpu.CompilerParams(collective_id=0, has_side_effects=True, vmem_limit_bytes=STEP_VMEM),
        cost_estimate=pl.CostEstimate(flops=12_000_000_000, bytes_accessed=30_000_000, transcendentals=0),
    )(latents.reshape(T, D), cotangent.reshape(T, D), ln_params, w_qkv, w_out.reshape(2, D, D), w_up, w_down)
    y, dx, gln, gqkv, gout, gup, gdown = pl.pallas_call(
        publish_kernel,
        out_shape=[jax.ShapeDtypeStruct(s, t) for s, t in shapes]
        + [jax.ShapeDtypeStruct(s, F32) for s in ((2, D, 3 * D), (2, D, D), (2, D, FF), (2, FF, D))],
        in_specs=[vmem_spec] * 4,
        out_specs=[any_spec] * 7,
        scratch_shapes=[dma((27,))],
        compiler_params=pltpu.CompilerParams(vmem_limit_bytes=2_000_000),
    )(*held)
    return (y.reshape(latents.shape), dx.reshape(latents.shape), gln, gqkv, gout.reshape(2, 6, 64, D), gup, gdown)


def solution(mesh):
    act_spec = P('data', 'sp', None, None)
    replicated = P()
    part_spec = P('data')
    return jax.shard_map(functools.partial(device_step, mesh.shape["sp"]), mesh=mesh,
                         in_specs=(act_spec, act_spec, replicated, replicated, replicated, replicated, replicated),
                         out_specs=(act_spec, act_spec, part_spec, part_spec, part_spec, part_spec, part_spec),
                         check_vma=False)
```

```python
import functools

import jax
import jax.numpy as jnp
from jax import lax
from jax.experimental import pallas as pl
from jax.experimental.pallas import tpu as pltpu
from jax.sharding import PartitionSpec as P

F32 = jnp.float32
BF16 = jnp.bfloat16
D = 384
T = 512
SEQ = 256
FF = 1536
ROWS = 128
MESH = pl.DeviceIdType.MESH
STEP_VMEM = 48_000_000
GELU_C = 0.7978845608028654
GELU_A = 0.044715


def dot_nn(a, b):
    return lax.dot_general(a, b, (((1,), (0,)), ((), ())), preferred_element_type=F32)


def dot_nt(a, b):
    return lax.dot_general(a, b, (((1,), (1,)), ((), ())), preferred_element_type=F32)


def dot_tn(a, b):
    return lax.dot_general(a, b, (((0,), (0,)), ((), ())), preferred_element_type=F32)


def run_events(i, events):
    for k, event in enumerate(events):
        if event is not None:
            pl.when(i == k)(event)


def row_tiles(body, events=()):
    def step(i, _):
        body(pl.ds(pl.multiple_of(i * ROWS, ROWS), ROWS))
        run_events(i, events)
        return 0
    lax.fori_loop(0, T // ROWS, step, 0)


def ln_norm(x32):
    mean = jnp.sum(x32, axis=-1, keepdims=True) * (1.0 / D)
    centered = x32 - mean
    inv_std = lax.rsqrt(jnp.sum(centered * centered, axis=-1, keepdims=True) * (1.0 / D) + 1e-6)
    return centered * inv_std, inv_std


def ln_back(d32, normed, inv_std, gain):
    d_norm = d32 * gain
    d_center = d_norm - jnp.sum(d_norm, axis=-1, keepdims=True) * (1.0 / D)
    return inv_std * (d_center - normed * (jnp.sum(d_norm * normed, axis=-1, keepdims=True) * (1.0 / D)))


def head_pairs(body, events=()):
    def step(i, _):
        seq = i // 3
        pair = i - seq * 3
        rows = pl.ds(pl.multiple_of(seq * SEQ, SEQ), SEQ)
        body(i, rows, pair)
        run_events(i, events)
        return 0
    lax.fori_loop(0, 6, step, 0)


def pair_cols(which, pair):
    return pl.ds(pl.multiple_of(which * D + pair * 128, 128), 128)


def attn_forward(x_ref, ln_ref, wqkv_ref, qkv_s, p_s, o_s):
    def qkv_tile(rows):
        normed, _ = ln_norm(x_ref[rows, :].astype(F32))
        a_in = (normed * ln_ref[0:1, :] + ln_ref[1:2, :]).astype(BF16)
        qkv_s[rows, :] = dot_nn(a_in, wqkv_ref[...]).astype(BF16)
    row_tiles(qkv_tile)

    def heads(i, rows, pair):
        q2 = qkv_s[rows, pair_cols(0, pair)]
        k2 = qkv_s[rows, pair_cols(1, pair)]
        v2 = qkv_s[rows, pair_cols(2, pair)]
        outs = []
        for e in range(2):
            cut = slice(e * 64, e * 64 + 64)
            scores = dot_nt(q2[:, cut], k2[:, cut]) * 0.125
            top = jnp.max(scores, axis=-1, keepdims=True)
            expd = jnp.exp(scores - top)
            total = jnp.sum(expd, axis=-1, keepdims=True)
            probs = (expd * (1.0 / total)).astype(BF16)
            p_s[i * 2 + e] = probs
            outs.append(dot_nn(probs, v2[:, cut]).astype(BF16))
        o_s[rows, pair_cols(0, pair)] = jnp.concatenate(outs, axis=1)
    head_pairs(heads)


def hidden(x_ref, o_s, wout_ref, h_s, rows):
    hid = (x_ref[rows, :].astype(F32) + dot_nn(o_s[rows, :], wout_ref[...])).astype(BF16)
    h_s[rows, :] = hid
    return hid.astype(F32)


def gelu_parts(up):
    up2 = up * up
    tanh = jnp.tanh(GELU_C * up * (1.0 + GELU_A * up2))
    half = 0.5 + 0.5 * tanh
    return up2, tanh, half


def mlp_forward(hid32, ln_ref, wup_ref, wdown_ref):
    normed, _ = ln_norm(hid32)
    m_in = (normed * ln_ref[2:3, :] + ln_ref[3:4, :]).astype(BF16)
    total = None
    for c in range(4):
        up = dot_nn(m_in, wup_ref[:, c * D:(c + 1) * D])
        act = (up * gelu_parts(up)[2]).astype(BF16)
        part = dot_nn(act, wdown_ref[c * D:(c + 1) * D, :])
        total = part if total is None else total + part
    return (hid32 + total).astype(BF16)


def mlp_backward(hid32, dy, ln_ref, wup_ref, wout_ref, wdown_ref, m_s, act_s, dup_s, dhid_s, datt_s, lng_ref, rows, emit):
    normed, inv_std = ln_norm(hid32)
    m_in = (normed * ln_ref[2:3, :] + ln_ref[3:4, :]).astype(BF16)
    m_s[rows, :] = m_in
    total = None
    dm = None
    for c in range(4):
        cols = slice(c * D, (c + 1) * D)
        up = dot_nn(m_in, wup_ref[:, cols])
        up2, tanh, half = gelu_parts(up)
        act = (up * half).astype(BF16)
        act_s[rows, cols] = act
        if emit is not None:
            part = dot_nn(act, wdown_ref[cols, :])
            total = part if total is None else total + part
        slope = half + (0.5 * up) * (1.0 - tanh * tanh) * (GELU_C + (3.0 * GELU_A * GELU_C) * up2)
        d_act = dot_nt(dy, wdown_ref[cols, :]).astype(BF16).astype(F32)
        d_up = (d_act * slope).astype(BF16)
        dup_s[rows, cols] = d_up
        d_part = dot_nt(d_up, wup_ref[:, cols])
        dm = d_part if dm is None else dm + d_part
    if emit is not None:
        emit[rows, :] = (hid32 + total).astype(BF16)
    dm32 = dm.astype(BF16).astype(F32)
    lng_ref[2:3, :] += jnp.sum(dm32 * normed, axis=0, keepdims=True)
    lng_ref[3:4, :] += jnp.sum(dm32, axis=0, keepdims=True)
    d_hid32 = ln_back(dm32, normed, inv_std, ln_ref[2:3, :])
    d_hid = (d_hid32 + dy.astype(F32)).astype(BF16)
    dhid_s[rows, :] = d_hid
    datt_s[rows, :] = dot_nt(d_hid, wout_ref[...]).astype(BF16)


def up_grad(g_ref, m_s, dup_s, c):
    g_ref[4 + c] = dot_tn(m_s[...], dup_s[:, pl.ds(pl.multiple_of(c * D, D), D)])


def down_grad(g_ref, act_s, dy_ref, c):
    g_ref[8 + c] = dot_tn(act_s[:, pl.ds(pl.multiple_of(c * D, D), D)], dy_ref[...])


def mlp_grads_first(g_ref, m_s, act_s, dup_s, dy_ref):
    def up(c, _):
        up_grad(g_ref, m_s, dup_s, c)
        return 0
    lax.fori_loop(0, 4, up, 0)

    def down(c, _):
        down_grad(g_ref, act_s, dy_ref, c)
        return 0
    lax.fori_loop(0, 2, down, 0)


def mlp_grads_last(g_ref, act_s, dhid_s, o_s, dy_ref):
    def down(c, _):
        down_grad(g_ref, act_s, dy_ref, c)
        return 0
    lax.fori_loop(2, 4, down, 0)
    g_ref[3] = dot_tn(o_s[...], dhid_s[...])


def attn_backward(qkv_s, p_s, datt_s, dqkv_s, events=()):
    def heads(i, rows, pair):
        q2 = qkv_s[rows, pair_cols(0, pair)]
        k2 = qkv_s[rows, pair_cols(1, pair)]
        v2 = qkv_s[rows, pair_cols(2, pair)]
        do2 = datt_s[rows, pair_cols(0, pair)]
        dqs, dks, dvs = [], [], []
        for e in range(2):
            cut = slice(e * 64, e * 64 + 64)
            probs = p_s[i * 2 + e]
            d_out = do2[:, cut]
            d_probs = dot_nt(d_out, v2[:, cut]).astype(BF16).astype(F32)
            p32 = probs.astype(F32)
            row_dot = jnp.sum(d_probs * p32, axis=-1, keepdims=True)
            d_scores = (p32 * (d_probs - row_dot) * 0.125).astype(BF16)
            dqs.append(dot_nn(d_scores, k2[:, cut]).astype(BF16))
            dks.append(dot_tn(d_scores, q2[:, cut]).astype(BF16))
            dvs.append(dot_tn(probs, d_out).astype(BF16))
        dqkv_s[rows, pair_cols(0, pair)] = jnp.concatenate(dqs, axis=1)
        dqkv_s[rows, pair_cols(1, pair)] = jnp.concatenate(dks, axis=1)
        dqkv_s[rows, pair_cols(2, pair)] = jnp.concatenate(dvs, axis=1)
    head_pairs(heads, events)


def qkv_backward(x_ref, dqkv_s, dhid_s, ln_ref, wqkv_ref, a_s, dx_ref, lng_ref):
    def tile(rows):
        normed, inv_std = ln_norm(x_ref[rows, :].astype(F32))
        a_s[rows, :] = (normed * ln_ref[0:1, :] + ln_ref[1:2, :]).astype(BF16)
        da32 = dot_nt(dqkv_s[rows, :], wqkv_ref[...]).astype(BF16).astype(F32)
        lng_ref[0:1, :] += jnp.sum(da32 * normed, axis=0, keepdims=True)
        lng_ref[1:2, :] += jnp.sum(da32, axis=0, keepdims=True)
        d_in = ln_back(da32, normed, inv_std, ln_ref[0:1, :])
        dx_ref[rows, :] = (d_in + dhid_s[rows, :].astype(F32)).astype(BF16)
    row_tiles(tile)


def qkv_grads(g_ref, a_s, dqkv_s):
    def chunk(c, _):
        g_ref[c] = dot_tn(a_s[...], dqkv_s[:, pl.ds(pl.multiple_of(c * D, D), D)])
        return 0
    lax.fori_loop(0, 3, chunk, 0)


def to_pieces(act_s, snd_ref):
    for a in range(2):
        snd_ref[:, a] = act_s[a * SEQ:(a + 1) * SEQ, :].reshape(SEQ // 2, 2, D)


def from_pieces(rcv_ref, dst_ref):
    flat = rcv_ref[...].reshape(T, D)
    row = lax.broadcasted_iota(jnp.int32, (SEQ, T), 0)
    col = lax.broadcasted_iota(jnp.int32, (SEQ, T), 1)
    for b in range(2):
        pick = (col == 2 * row + b).astype(F32).astype(BF16)
        dst_ref[b * SEQ:(b + 1) * SEQ, :] = dot_nn(pick, flat).astype(BF16)


EXCHANGE = 24
ROUND_BLOCKS = ((4, 5, 6, 7, 8, 9), (10, 11, 3, 0, 1, 2), (4, 5, 6, 7, 8, 9), (10, 11, 3), (0, 1, 2))
ROUND_SIDE = (1, 1, 0, 0, 0)


def round_sizes(blocks):
    keep = rows = D * len(blocks) // 12
    sizes = []
    while rows > EXCHANGE:
        rows //= 2
        sizes.append(rows)
    return keep, len(sizes), sizes + [EXCHANGE] * (6 - len(sizes))


def dim_info(me, dim):
    axis, far = dim // 2, dim % 2
    stride = (2, 8, 32)[axis]
    coord = lax.rem(lax.div(me, stride), 4)
    if far:
        bit = lax.div(coord, 2)
        partner = me + (3 - 2 * coord) * stride
    else:
        bit = lax.rem(coord + lax.div(coord, 2), 2)
        partner = me + (1 - 2 * lax.rem(coord, 2)) * stride
    return bit, partner


def remote_copy(src, dst, s_sem, r_sem, to):
    return pltpu.make_async_remote_copy(src, dst, s_sem, r_sem, device_id={"sp": to}, device_id_type=MESH)


def rows_at(start, size):
    return pl.ds(pl.multiple_of(start, 8), size)


class Round:
    def __init__(self, index, grads, me, dims, half, recv, sems):
        self.r = index
        self.g = grads.at[ROUND_SIDE[index]]
        self.keep, self.halvings, self.sizes = round_sizes(ROUND_BLOCKS[index])
        self.dims = dims
        self.half = half
        self.recv = recv
        core = lax.rem(me, 2)
        self.sibling = me + 1 - 2 * core
        (self.half_send, self.half_recv, self.send_sem, self.recv_sem, self.back_send, self.back_recv,
         self.fwd_send, self.fwd_recv, self.free_sem, self.core_free) = sems
        per_block = 6 // len(ROUND_BLOCKS[index])
        self.block = [ROUND_BLOCKS[index][p // per_block] for p in range(6)]
        first = [2 * self.keep * (p % per_block) for p in range(6)]
        self.away = [first[p] + (1 - core) * self.keep for p in range(6)]
        self.offs = {(p, 0): first[p] + core * self.keep for p in range(6)}
        self.give = {}
        for p in range(6):
            for t in range(6):
                off, size, bit = self.offs[p, t], self.sizes[t], dims[(p + t) % 6][0]
                halve = t < self.halvings
                self.offs[p, t + 1] = off + bit * size if halve else off
                self.give[p, t] = off + (1 - bit) * size if halve else off

    def rows(self, p, off, size):
        return self.g.at[self.block[p], rows_at(off, size)]

    def partner(self, t, p):
        return self.dims[(p + t) % 6][1]

    def core_copy(self, p):
        return remote_copy(self.rows(p, self.away[p], self.keep), self.half.at[p], self.half_send.at[self.r],
                           self.half_recv.at[self.r], self.sibling)

    def recv_rows(self, t):
        return pl.ds(sum(self.sizes[:t]), self.sizes[t])

    def send_copy(self, t, p):
        return remote_copy(self.rows(p, self.give[p, t], self.sizes[t]), self.recv.at[p, self.recv_rows(t)],
                           self.send_sem.at[self.r], self.recv_sem.at[self.r, t], self.partner(t, p))

    def back_copy(self, t, p):
        rows = self.rows(p, self.offs[p, t + 1], self.sizes[t])
        return remote_copy(rows, rows, self.back_send.at[self.r], self.back_recv.at[self.r, t], self.partner(t, p))

    def forward_copy(self, slot, p):
        last = self.halvings
        if slot == 0:
            rows = self.rows(p, self.offs[p, last], self.sizes[last - 1])
        else:
            rows = self.rows(p, self.give[p, last - slot], self.sizes[last - slot])
        return remote_copy(rows, rows, self.fwd_send.at[self.r], self.fwd_recv.at[self.r], self.sibling)

    def wait_bytes(self, ref, *semaphores):
        for sem in semaphores:
            pltpu.make_async_copy(ref, ref, sem).wait()

    def start_core(self):
        for p in range(6):
            self.core_copy(p).start()

    def join_core(self):
        self.wait_bytes(self.half, self.half_send.at[self.r], self.half_recv.at[self.r])
        pl.semaphore_signal(self.core_free.at[self.r], inc=1, device_id={"sp": self.sibling}, device_id_type=MESH)
        for p in range(6):
            self.g[self.block[p], rows_at(self.offs[p, 0], self.keep)] += self.half[p]
            self.send_copy(0, p).start()

    def start_back(self, t):
        pl.semaphore_wait(self.free_sem.at[self.r, t], 6)
        for p in range(6):
            self.back_copy(t, p).start()

    def step(self, t):
        size = self.sizes[t]
        self.wait_bytes(self.recv.at[:, self.recv_rows(t)], self.send_sem.at[self.r], self.recv_sem.at[self.r, t])
        for p in range(6):
            if t < self.halvings:
                pl.semaphore_signal(self.free_sem.at[self.r, t], inc=1, device_id={"sp": self.partner(t, p)},
                                    device_id_type=MESH)
            self.g[self.block[p], rows_at(self.offs[p, t + 1], size)] += self.recv[p, self.recv_rows(t)]
            if t < 5:
                self.send_copy(t + 1, p).start()
        if t == 5:
            self.start_back(self.halvings - 1)
            pl.semaphore_wait(self.core_free.at[self.r], 1)
            for p in range(6):
                self.forward_copy(0, p).start()

    def back(self, t):
        self.wait_bytes(self.recv.at[:, self.recv_rows(t)], self.back_send.at[self.r], self.back_recv.at[self.r, t])
        if t > 0:
            self.start_back(t - 1)
        for p in range(6):
            self.forward_copy(self.halvings - t, p).start()

    def finish(self):
        self.wait_bytes(self.half, self.fwd_send.at[self.r], self.fwd_recv.at[self.r])


def out_slices(blk, gqkv, gout, gup, gdown):
    cols = [pl.ds(c * D, D) for c in range(4)]
    return ([gqkv.at[blk, :, cols[c]] for c in range(3)] + [gout.at[blk]] + [gup.at[blk, :, cols[c]] for c in range(4)]
            + [gdown.at[blk, cols[c]] for c in range(4)])


def step_kernel(n, x_hbm, cot_hbm, ln_in, wqkv_hbm, wout_hbm, wup_hbm, wdown_hbm,
                y_ref, dx_ref, gln_ref, grads,
                x_s, cot_s, mid_s, dmid_s, act_a, ln_s, wqkv, wout, wup, wdown, qkv_s, p_s, o_s, h_s,
                m_s, act_s, dup_s, dhid_s, datt_s, dqkv_s, a_s, snd, rcv, lnacc, lnrecv, *rest):
    halves, recvs = rest[:5], rest[5:10]
    (load_sem, swap_send, swap_recv, swap_local, *sems) = rest[10:]
    me = lax.axis_index("sp")
    dims = [dim_info(me, d) for d in range(6)]
    sibling = me + 1 - 2 * lax.rem(me, 2)
    ln_send, ln_recv = sems[-2:]
    sems = sems[:-2]

    barrier = pltpu.get_barrier_semaphore()

    def greet(k, _):
        pl.semaphore_signal(barrier, inc=1, device_id={"sp": lax.rem(me + k, n)}, device_id_type=MESH)
        return 0
    lax.fori_loop(1, n, greet, 0)

    loads = {}
    for name, src, dst in (("x", x_hbm, x_s), ("qkv0", wqkv_hbm.at[0], wqkv.at[0]), ("cot", cot_hbm, cot_s),
                           ("out0", wout_hbm.at[0], wout.at[0]), ("up0", wup_hbm.at[0], wup.at[0]),
                           ("down0", wdown_hbm.at[0], wdown.at[0]), ("qkv1", wqkv_hbm.at[1], wqkv.at[1]),
                           ("out1", wout_hbm.at[1], wout.at[1]), ("up1", wup_hbm.at[1], wup.at[1]),
                           ("down1", wdown_hbm.at[1], wdown.at[1])):
        loads[name] = pltpu.make_async_copy(src, dst, load_sem.at[len(loads)])
        loads[name].start()

    def need(*names):
        for name in names:
            loads[name].wait()

    def remote_piece(i, k):
        to = lax.rem(me + k, n)
        return remote_copy(snd.at[i, to], rcv.at[i, me], swap_send.at[i], swap_recv.at[i], to)

    def start_swap(i):
        pltpu.make_async_copy(snd.at[i, me], rcv.at[i, me], swap_local.at[i]).start()

        def send(k, _):
            remote_piece(i, k).start()
            return 0
        lax.fori_loop(1, n, send, 0)

    def end_swap(i):
        pltpu.make_async_copy(snd.at[i, me], rcv.at[i, me], swap_local.at[i]).wait()
        rest = pl.ds(0, n - 1)
        pltpu.make_async_copy(snd.at[i, rest], rcv.at[i, rest], swap_send.at[i]).wait()
        pltpu.make_async_copy(snd.at[i, rest], rcv.at[i, rest], swap_recv.at[i]).wait()

    ln_s[...] = ln_in[...].astype(F32)
    lnacc[...] = jnp.zeros_like(lnacc)
    ln = [ln_s.at[i] for i in range(2)]
    lng = [lnacc.at[pl.ds(8 * i, 8)] for i in range(2)]
    saved = [(qkv_s.at[i], p_s.at[i], o_s.at[i]) for i in range(2)]
    rounds = [Round(r, grads, me, dims, halves[r], recvs[r], sems) for r in range(5)]
    r1, r2, r3, r4, r5 = rounds

    need("x", "qkv0")
    attn_forward(x_s, ln[0], wqkv.at[0], *saved[0])
    need("cot")
    to_pieces(cot_s, snd.at[0])
    need("out0", "up0", "down0")

    def spatial_tail(rows):
        hid32 = hidden(x_s, o_s.at[0], wout.at[0], h_s.at[0], rows)
        mid_s[rows, :] = mlp_forward(hid32, ln[0], wup.at[0], wdown.at[0])
    row_tiles(spatial_tail)
    to_pieces(mid_s, snd.at[1])
    pl.semaphore_wait(barrier, n - 1)
    start_swap(1)
    start_swap(0)

    need("qkv1", "out1", "up1", "down1")
    end_swap(1)
    from_pieces(rcv.at[1], mid_s)
    attn_forward(mid_s, ln[1], wqkv.at[1], *saved[1])
    end_swap(0)
    from_pieces(rcv.at[0], cot_s)

    def temporal_tail(rows):
        hid32 = hidden(mid_s, o_s.at[1], wout.at[1], h_s.at[1], rows)
        mlp_backward(hid32, cot_s[rows, :], ln[1], wup.at[1], wout.at[1], wdown.at[1], m_s, act_s, dup_s, dhid_s, datt_s,
                     lng[1], rows, act_a)
    row_tiles(temporal_tail)
    to_pieces(act_a, snd.at[2])
    start_swap(2)
    mlp_grads_first(grads.at[1], m_s, act_s, dup_s, cot_s)
    r1.start_core()
    attn_backward(qkv_s.at[1], p_s.at[1], datt_s, dqkv_s, (None, None, r1.join_core))
    qkv_backward(mid_s, dqkv_s, dhid_s, ln[1], wqkv.at[1], a_s, dmid_s, lng[1])
    to_pieces(dmid_s, snd.at[3])
    start_swap(3)
    mlp_grads_last(grads.at[1], act_s, dhid_s, o_s.at[1], cot_s)
    qkv_grads(grads.at[1], a_s, dqkv_s)
    r2.start_core()
    r1.step(0)
    end_swap(2)
    from_pieces(rcv.at[2], y_ref)
    r2.join_core()
    r1.step(1)
    end_swap(3)
    from_pieces(rcv.at[3], dmid_s)

    def back_tail(rows):
        mlp_backward(h_s[0, rows, :].astype(F32), dmid_s[rows, :], ln[0], wup.at[0], wout.at[0], wdown.at[0], m_s, act_s,
                     dup_s, dhid_s, datt_s, lng[0], rows, None)

    def both(*steps):
        def event():
            for method, *args in steps:
                method(*args)
        return event

    row_tiles(back_tail, (both((r1.step, 2)), None, both((r1.step, 3), (r2.step, 0)), None))
    mlp_grads_first(grads.at[0], m_s, act_s, dup_s, dmid_s)
    r3.start_core()
    r1.step(4)
    r2.step(1)
    mlp_grads_last(grads.at[0], act_s, dhid_s, o_s.at[0], dmid_s)
    r4.start_core()
    attn_backward(qkv_s.at[0], p_s.at[0], datt_s, dqkv_s, (
        both((r3.join_core,), (r1.step, 5)), both((r2.step, 2),), both((r4.join_core,)), both((r1.back, 2)),
        both((r2.step, 3)), both((r3.step, 0))))
    qkv_backward(x_s, dqkv_s, dhid_s, ln[0], wqkv.at[0], a_s, dx_ref, lng[0])
    def ln_copy(t):
        to = sibling if t == 0 else dims[t - 1][1]
        return remote_copy(lnacc, lnrecv.at[t], ln_send.at[0], ln_recv.at[t], to)

    def ln_next(t):
        ln_copy(t).wait()
        lnacc[...] += lnrecv[t]
        if t < 6:
            ln_copy(t + 1).start()

    ln_copy(0).start()
    qkv_grads(grads.at[0], a_s, dqkv_s)
    r5.start_core()
    r2.step(4)
    r4.step(0)
    r1.back(1)
    r3.step(1)
    ln_next(0)
    r5.join_core()
    r2.step(5)
    r4.step(1)
    r3.step(2)
    r1.back(0)
    r5.step(0)
    ln_next(1)
    r2.back(2)
    r3.step(3)
    r4.step(2)
    r5.step(1)
    ln_next(2)
    r2.back(1)
    r3.step(4)
    r4.step(3)
    r5.step(2)
    ln_next(3)
    r3.step(5)
    r4.step(4)
    r5.step(3)
    ln_next(4)
    r2.back(0)
    r3.back(2)
    r4.step(5)
    r5.step(4)
    ln_next(5)
    r3.back(1)
    r4.back(1)
    r5.step(5)
    ln_next(6)
    r5.back(1)
    r3.back(0)
    r4.back(0)
    r5.back(0)
    for i in range(2):
        gln_ref[i] = lnacc[8 * i:8 * i + 4, :]
    for rnd in rounds:
        rnd.finish()


def publish_kernel(y_in, dx_in, gln_in, grads, y_ref, dx_ref, gln_ref, gqkv, gout, gup, gdown, sem):
    pairs = [(y_in, y_ref), (dx_in, dx_ref), (gln_in, gln_ref)]
    for i in range(2):
        slices = out_slices(i, gqkv, gout, gup, gdown)
        pairs += [(grads.at[i, j], slices[j]) for j in range(12)]
    copies = [pltpu.make_async_copy(src, dst, sem.at[k]) for k, (src, dst) in enumerate(pairs)]
    for copy in copies:
        copy.start()
    for copy in copies:
        copy.wait()


def device_step(n, latents, cotangent, ln_params, w_qkv, w_out, w_up, w_down):
    dma = pltpu.SemaphoreType.DMA
    regular = pltpu.SemaphoreType.REGULAR
    any_spec = pl.BlockSpec(memory_space=pl.ANY)
    vmem_spec = pl.BlockSpec(memory_space=pltpu.VMEM)
    act, wide, qkv = (T, D), (T, FF), (T, 3 * D)
    shapes = [(act, BF16), (act, BF16), ((2, 4, D), F32)]
    held = pl.pallas_call(
        functools.partial(step_kernel, n),
        out_shape=[pltpu.VMEM(s, t) for s, t in shapes] + [pltpu.VMEM((2, 12, D, D), F32)],
        in_specs=[any_spec, any_spec, vmem_spec] + [any_spec] * 4,
        out_specs=[vmem_spec] * 4,
        scratch_shapes=[pltpu.VMEM(s, BF16) for s in [act] * 5]
        + [pltpu.VMEM((2, 4, D), F32)]
        + [pltpu.VMEM((2,) + s, BF16) for s in ((D, 3 * D), (D, D), (D, FF), (FF, D), qkv, (12, SEQ, SEQ), act, act)]
        + [pltpu.VMEM(s, BF16) for s in (act, wide, wide, act, act, qkv, act)]
        + [pltpu.VMEM((4, n, 2, 2, D), BF16)] * 2
        + [pltpu.VMEM((16, D), F32), pltpu.VMEM((7, 16, D), F32)]
        + [pltpu.VMEM((6, round_sizes(blocks)[0], D), F32) for blocks in ROUND_BLOCKS]
        + [pltpu.VMEM((6, sum(round_sizes(blocks)[2]), D), F32) for blocks in ROUND_BLOCKS]
        + [dma((10,)), dma((4,)), dma((4,)), dma((4,))]
        + [dma((5,)), dma((5,)), dma((5,)), dma((5, 6)), dma((5,)), dma((5, 3)), dma((5,)), dma((5,)), regular((5, 3)),
           regular((5,)), dma((1,)), dma((7,))],
        compiler_params=pltpu.CompilerParams(collective_id=0, has_side_effects=True, vmem_limit_bytes=STEP_VMEM),
        cost_estimate=pl.CostEstimate(flops=12_000_000_000, bytes_accessed=30_000_000, transcendentals=0),
    )(latents.reshape(T, D), cotangent.reshape(T, D), ln_params, w_qkv, w_out.reshape(2, D, D), w_up, w_down)
    y, dx, gln, gqkv, gout, gup, gdown = pl.pallas_call(
        publish_kernel,
        out_shape=[jax.ShapeDtypeStruct(s, t) for s, t in shapes]
        + [jax.ShapeDtypeStruct(s, F32) for s in ((2, D, 3 * D), (2, D, D), (2, D, FF), (2, FF, D))],
        in_specs=[vmem_spec] * 4,
        out_specs=[any_spec] * 7,
        scratch_shapes=[dma((27,))],
        compiler_params=pltpu.CompilerParams(vmem_limit_bytes=2_000_000),
    )(*held)
    return (y.reshape(latents.shape), dx.reshape(latents.shape), gln, gqkv, gout.reshape(2, 6, 64, D), gup, gdown)


def solution(mesh):
    act_spec = P('data', 'sp', None, None)
    replicated = P()
    part_spec = P('data')
    return jax.shard_map(functools.partial(device_step, mesh.shape["sp"]), mesh=mesh,
                         in_specs=(act_spec, act_spec, replicated, replicated, replicated, replicated, replicated),
                         out_specs=(act_spec, act_spec, part_spec, part_spec, part_spec, part_spec, part_spec),
                         check_vma=False)
```

```python
import functools

import jax
import jax.numpy as jnp
from jax import lax
from jax.experimental import pallas as pl
from jax.experimental.pallas import tpu as pltpu
from jax.sharding import PartitionSpec as P

F32 = jnp.float32
BF16 = jnp.bfloat16
D = 384
T = 512
SEQ = 256
FF = 1536
WIDTH = 256
MESH = pl.DeviceIdType.MESH
STEP_VMEM = 51_500_000
GELU_C = 0.7978845608028654
GELU_A = 0.044715


def dot_nn(a, b):
    return lax.dot_general(a, b, (((1,), (0,)), ((), ())), preferred_element_type=F32)


def dot_nt(a, b):
    return lax.dot_general(a, b, (((1,), (1,)), ((), ())), preferred_element_type=F32)


def dot_tn(a, b):
    return lax.dot_general(a, b, (((0,), (0,)), ((), ())), preferred_element_type=F32)


def ln_norm(x32):
    mean = jnp.sum(x32, axis=-1, keepdims=True) * (1.0 / D)
    centered = x32 - mean
    inv_std = lax.rsqrt(jnp.sum(centered * centered, axis=-1, keepdims=True) * (1.0 / D) + 1e-6)
    return centered * inv_std, inv_std


def ln_back(d32, normed, inv_std, gain):
    d_norm = d32 * gain
    d_center = d_norm - jnp.sum(d_norm, axis=-1, keepdims=True) * (1.0 / D)
    return inv_std * (d_center - normed * (jnp.sum(d_norm * normed, axis=-1, keepdims=True) * (1.0 / D)))


def seq_loop(body, between=None):
    def step(seq, _):
        body(seq, pl.ds(pl.multiple_of(seq * SEQ, SEQ), SEQ))
        if between is not None:
            pl.when(seq == 0)(between)
        return 0
    lax.fori_loop(0, 2, step, 0)


HEAD_CUTS = (slice(0, 64), slice(64, 128))
SCORE_EXP2 = 0.125 * 1.4426950408889634


def pair_cols(which, pair):
    return slice(which * D + pair * 128, which * D + (pair + 1) * 128)


def attn_forward(x_ref, ln_ref, wqkv_ref, qkv_s, p_s, o_s):
    normed, _ = ln_norm(x_ref[...].astype(F32))
    a_in = (normed * ln_ref[0:1, :] + ln_ref[1:2, :]).astype(BF16)
    qkv_s[...] = dot_nn(a_in, wqkv_ref[...]).astype(BF16)

    def heads(seq, rows):
        for pair in range(3):
            q2, k2, v2 = (qkv_s[rows, pair_cols(which, pair)] for which in range(3))
            scores = [dot_nt(q2[:, cut], k2[:, cut]) for cut in HEAD_CUTS]
            outs = []
            for e in range(2):
                top = jnp.max(scores[e], axis=-1, keepdims=True)
                expd = jnp.exp2((scores[e] - top) * SCORE_EXP2)
                total = jnp.sum(expd, axis=-1, keepdims=True)
                probs = (expd * (1.0 / total)).astype(BF16)
                p_s[seq * 6 + pair * 2 + e] = probs
                outs.append(probs)
            o_s[rows, pair_cols(0, pair)] = jnp.concatenate(
                [dot_nn(outs[e], v2[:, HEAD_CUTS[e]]).astype(BF16) for e in range(2)], axis=1)
    seq_loop(heads)


def hidden(x_ref, o_s, wout_ref):
    hid = (x_ref[...].astype(F32) + dot_nn(o_s[...], wout_ref[...])).astype(BF16)
    return hid


def gelu_parts(up):
    up2 = up * up
    tanh = jnp.tanh(GELU_C * up * (1.0 + GELU_A * up2))
    half = 0.5 + 0.5 * tanh
    return up2, tanh, half


def ff_cols():
    return [slice(c, c + WIDTH) for c in range(0, FF, WIDTH)]


def gelu_slope(up, up2, tanh, half):
    return half + (0.5 * up) * (1.0 - tanh * tanh) * (GELU_C + (3.0 * GELU_A * GELU_C) * up2)


def mlp_input(hid32, ln_ref):
    normed, inv_std = ln_norm(hid32)
    return (normed * ln_ref[2:3, :] + ln_ref[3:4, :]).astype(BF16), normed, inv_std


def mlp_forward(hid32, ln_ref, wup_ref, wdown_ref, act_s):
    m_in, _, _ = mlp_input(hid32, ln_ref)
    for cols in ff_cols():
        up = dot_nn(m_in, wup_ref[:, cols])
        act_s[:, cols] = (up * gelu_parts(up)[2]).astype(BF16)
    return (hid32 + dot_nn(act_s[...], wdown_ref[...])).astype(BF16)


def hidden_backward(dm, normed, inv_std, dy, ln_ref, wout_ref, dhid_s, datt_s, lng_ref, rows):
    dm32 = dm.astype(BF16).astype(F32)
    lng_ref[2:3, :] += jnp.sum(dm32 * normed, axis=0, keepdims=True)
    lng_ref[3:4, :] += jnp.sum(dm32, axis=0, keepdims=True)
    d_hid32 = ln_back(dm32, normed, inv_std, ln_ref[2:3, :])
    d_hid = (d_hid32 + dy.astype(F32)).astype(BF16)
    dhid_s[rows, :] = d_hid
    datt_s[rows, :] = dot_nt(d_hid, wout_ref[...]).astype(BF16)


def mlp_both_ways(hid32, dy_ref, ln_ref, wup_ref, wout_ref, wdown_ref, m_s, act_s, dup_s, dhid_s, datt_s, lng_ref, out_ref):
    m_in, normed, inv_std = mlp_input(hid32, ln_ref)
    m_s[...] = m_in
    dy = dy_ref[...]
    total = None
    dm = None
    for cols in ff_cols():
        up = dot_nn(m_in, wup_ref[:, cols])
        up2, tanh, half = gelu_parts(up)
        act = (up * half).astype(BF16)
        act_s[:, cols] = act
        part = dot_nn(act, wdown_ref[cols, :])
        total = part if total is None else total + part
        d_act = dot_nt(dy, wdown_ref[cols, :]).astype(BF16).astype(F32)
        d_up = (d_act * gelu_slope(up, up2, tanh, half)).astype(BF16)
        dup_s[:, cols] = d_up
        d_part = dot_nt(d_up, wup_ref[:, cols])
        dm = d_part if dm is None else dm + d_part
    out_ref[...] = (hid32 + total).astype(BF16)
    hidden_backward(dm, normed, inv_std, dy, ln_ref, wout_ref, dhid_s, datt_s, lng_ref, pl.ds(0, T))


def mlp_prepare(h_s, ln_ref, wup_ref, m_s, act_s, slope_ref):
    def tile(i, rows):
        m_in, _, _ = mlp_input(h_s[rows, :].astype(F32), ln_ref)
        m_s[rows, :] = m_in
        for c, cols in enumerate(ff_cols()):
            up = dot_nn(m_in, wup_ref[:, cols])
            up2, tanh, half = gelu_parts(up)
            act_s[rows, cols] = (up * half).astype(BF16)
            slope_ref[i * 6 + c, 0:SEQ, 0:WIDTH] = gelu_slope(up, up2, tanh, half)
    seq_loop(tile)


def mlp_backward(h_s, dy_ref, slope_ref, ln_ref, wup_ref, wout_ref, wdown_ref, dup_s, dhid_s, datt_s, lng_ref, between):
    def tile(i, rows):
        dy = dy_ref[rows, :]
        for c, cols in enumerate(ff_cols()):
            d_act = dot_nt(dy, wdown_ref[cols, :]).astype(BF16).astype(F32)
            dup_s[rows, cols] = (d_act * slope_ref[i * 6 + c, 0:SEQ, 0:WIDTH]).astype(BF16)
        normed, inv_std = ln_norm(h_s[rows, :].astype(F32))
        hidden_backward(dot_nt(dup_s[rows, :], wup_ref[...]), normed, inv_std, dy, ln_ref, wout_ref, dhid_s, datt_s, lng_ref,
                        rows)
    seq_loop(tile, between)


def mlp_grads_first(g_ref, m_s, act_s, dup_s, dy_ref):
    up = dot_tn(m_s[...], dup_s[...])
    for c in range(4):
        g_ref[4 + c] = up[:, c * D:(c + 1) * D]
    down = dot_tn(act_s[:, 0:2 * D], dy_ref[...])
    for c in range(2):
        g_ref[8 + c] = down[c * D:(c + 1) * D, :]


def mlp_grads_last(g_ref, act_s, dhid_s, o_s, dy_ref):
    down = dot_tn(act_s[:, 2 * D:4 * D], dy_ref[...])
    for c in range(2):
        g_ref[10 + c] = down[c * D:(c + 1) * D, :]
    g_ref[3] = dot_tn(o_s[...], dhid_s[...])


def attn_backward(qkv_s, p_s, datt_s, dqkv_s, between):
    def heads(seq, rows):
        for pair in range(3):
            q2, k2, v2 = (qkv_s[rows, pair_cols(which, pair)] for which in range(3))
            do2 = datt_s[rows, pair_cols(0, pair)]
            base = seq * 6 + pair * 2
            d_probs = [dot_nt(do2[:, cut], v2[:, cut]) for cut in HEAD_CUTS]
            d_value = [dot_tn(p_s[base + e], do2[:, HEAD_CUTS[e]]).astype(BF16) for e in range(2)]
            d_scores = []
            for e in range(2):
                d32 = d_probs[e].astype(BF16).astype(F32)
                p32 = p_s[base + e].astype(F32)
                row_dot = jnp.sum(d32 * p32, axis=-1, keepdims=True)
                d_scores.append((p32 * (d32 - row_dot) * 0.125).astype(BF16))
            d_query = [dot_nn(d_scores[e], k2[:, HEAD_CUTS[e]]).astype(BF16) for e in range(2)]
            d_key = [dot_tn(d_scores[e], q2[:, HEAD_CUTS[e]]).astype(BF16) for e in range(2)]
            for which, parts in enumerate((d_query, d_key, d_value)):
                dqkv_s[rows, pair_cols(which, pair)] = jnp.concatenate(parts, axis=1)
    seq_loop(heads, between)


def qkv_backward(x_ref, dqkv_s, dhid_s, ln_ref, wqkv_ref, a_s, dx_ref, lng_ref):
    normed, inv_std = ln_norm(x_ref[...].astype(F32))
    a_s[...] = (normed * ln_ref[0:1, :] + ln_ref[1:2, :]).astype(BF16)
    da32 = dot_nt(dqkv_s[...], wqkv_ref[...]).astype(BF16).astype(F32)
    lng_ref[0:1, :] += jnp.sum(da32 * normed, axis=0, keepdims=True)
    lng_ref[1:2, :] += jnp.sum(da32, axis=0, keepdims=True)
    d_in = ln_back(da32, normed, inv_std, ln_ref[0:1, :])
    dx_ref[...] = (d_in + dhid_s[...].astype(F32)).astype(BF16)


def qkv_grads(g_ref, a_s, dqkv_s):
    out = dot_tn(a_s[...], dqkv_s[...])
    for c in range(3):
        g_ref[c] = out[:, c * D:(c + 1) * D]


def to_pieces(act_s, snd_ref):
    for a in range(2):
        snd_ref[:, a] = act_s[a * SEQ:(a + 1) * SEQ, :].reshape(SEQ // 2, 2, D)


def from_pieces(rcv_ref, dst_ref):
    flat = rcv_ref[...].reshape(T, D)
    row = lax.broadcasted_iota(jnp.int32, (SEQ, T), 0)
    col = lax.broadcasted_iota(jnp.int32, (SEQ, T), 1)
    for b in range(2):
        pick = (col == 2 * row + b).astype(F32).astype(BF16)
        dst_ref[b * SEQ:(b + 1) * SEQ, :] = dot_nn(pick, flat).astype(BF16)


EXCHANGE = 24
ROUND_BLOCKS = ((4, 5, 6, 7, 8, 9), (10, 11, 3, 0, 1, 2), (4, 5, 6, 7, 8, 9), (10, 11, 3, 0, 1, 2))
ROUND_SIDE = (1, 1, 0, 0)
ROUNDS = len(ROUND_SIDE)
SCHEDULE = {
    "b": "",
    "c0": "",
    "c1": "1",
    "e": "",
    "f": "12",
    "h0": "",
    "h1": "",
    "i": "1",
    "j": "",
    "k0": "2",
    "k1": "13",
    "l": "",
    "tail": "2514321543215432145321435214352435243434",
}


def round_sizes(blocks):
    keep = rows = D * len(blocks) // 12
    sizes = []
    while rows > EXCHANGE:
        rows //= 2
        sizes.append(rows)
    return keep, len(sizes), sizes + [EXCHANGE] * (6 - len(sizes))


def dim_info(me, dim):
    axis, far = dim // 2, dim % 2
    stride = (2, 8, 32)[axis]
    coord = lax.rem(lax.div(me, stride), 4)
    if far:
        bit = lax.div(coord, 2)
        partner = me + (3 - 2 * coord) * stride
    else:
        bit = lax.rem(coord + lax.div(coord, 2), 2)
        partner = me + (1 - 2 * lax.rem(coord, 2)) * stride
    return bit, partner


def remote_copy(src, dst, s_sem, r_sem, to):
    return pltpu.make_async_remote_copy(src, dst, s_sem, r_sem, device_id={"sp": to}, device_id_type=MESH)


def rows_at(start, size):
    return pl.ds(pl.multiple_of(start, 8), size)


class Round:
    def __init__(self, index, grads, me, dims, half, recv, sems):
        self.r = index
        self.g = grads.at[ROUND_SIDE[index]]
        self.keep, self.halvings, self.sizes = round_sizes(ROUND_BLOCKS[index])
        self.dims = dims
        self.half = half
        self.recv = recv
        core = lax.rem(me, 2)
        self.sibling = me + 1 - 2 * core
        (self.half_send, self.half_recv, self.send_sem, self.recv_sem, self.back_send, self.back_recv,
         self.fwd_send, self.fwd_recv, self.free_sem, self.core_free) = sems
        per_block = 6 // len(ROUND_BLOCKS[index])
        self.block = [ROUND_BLOCKS[index][p // per_block] for p in range(6)]
        first = [2 * self.keep * (p % per_block) for p in range(6)]
        self.away = [first[p] + (1 - core) * self.keep for p in range(6)]
        self.offs = {(p, 0): first[p] + core * self.keep for p in range(6)}
        self.give = {}
        for p in range(6):
            for t in range(6):
                off, size, bit = self.offs[p, t], self.sizes[t], dims[(p + t) % 6][0]
                halve = t < self.halvings
                self.offs[p, t + 1] = off + bit * size if halve else off
                self.give[p, t] = off + (1 - bit) * size if halve else off

    def rows(self, p, off, size):
        return self.g.at[self.block[p], rows_at(off, size)]

    def partner(self, t, p):
        return self.dims[(p + t) % 6][1]

    def core_copy(self, p):
        return remote_copy(self.rows(p, self.away[p], self.keep), self.half.at[p], self.half_send.at[self.r],
                           self.half_recv.at[self.r], self.sibling)

    def recv_rows(self, t):
        return pl.ds(sum(self.sizes[:t]), self.sizes[t])

    def send_copy(self, t, p):
        return remote_copy(self.rows(p, self.give[p, t], self.sizes[t]), self.recv.at[p, self.recv_rows(t)],
                           self.send_sem.at[self.r], self.recv_sem.at[self.r, t], self.partner(t, p))

    def back_copy(self, t, p):
        rows = self.rows(p, self.offs[p, t + 1], self.sizes[t])
        return remote_copy(rows, rows, self.back_send.at[self.r], self.back_recv.at[self.r, t], self.partner(t, p))

    def forward_copy(self, slot, p):
        last = self.halvings
        if slot == 0:
            rows = self.rows(p, self.offs[p, last], self.sizes[last - 1])
        else:
            rows = self.rows(p, self.give[p, last - slot], self.sizes[last - slot])
        return remote_copy(rows, rows, self.fwd_send.at[self.r], self.fwd_recv.at[self.r], self.sibling)

    def wait_bytes(self, ref, *semaphores):
        for sem in semaphores:
            pltpu.make_async_copy(ref, ref, sem).wait()

    def start_core(self):
        for p in range(6):
            self.core_copy(p).start()

    def join_core(self):
        self.wait_bytes(self.half, self.half_send.at[self.r], self.half_recv.at[self.r])
        pl.semaphore_signal(self.core_free.at[self.r], inc=1, device_id={"sp": self.sibling}, device_id_type=MESH)
        for p in range(6):
            self.g[self.block[p], rows_at(self.offs[p, 0], self.keep)] += self.half[p]
            self.send_copy(0, p).start()

    def start_back(self, t):
        pl.semaphore_wait(self.free_sem.at[self.r, t], 6)
        for p in range(6):
            self.back_copy(t, p).start()

    def step(self, t):
        size = self.sizes[t]
        self.wait_bytes(self.recv.at[:, self.recv_rows(t)], self.send_sem.at[self.r], self.recv_sem.at[self.r, t])
        for p in range(6):
            if t < self.halvings:
                pl.semaphore_signal(self.free_sem.at[self.r, t], inc=1, device_id={"sp": self.partner(t, p)},
                                    device_id_type=MESH)
            self.g[self.block[p], rows_at(self.offs[p, t + 1], size)] += self.recv[p, self.recv_rows(t)]
            if t < 5:
                self.send_copy(t + 1, p).start()
        if t == 5:
            self.start_back(self.halvings - 1)
            pl.semaphore_wait(self.core_free.at[self.r], 1)
            for p in range(6):
                self.forward_copy(0, p).start()

    def back(self, t):
        self.wait_bytes(self.recv.at[:, self.recv_rows(t)], self.back_send.at[self.r], self.back_recv.at[self.r, t])
        if t > 0:
            self.start_back(t - 1)
        for p in range(6):
            self.forward_copy(self.halvings - t, p).start()

    def steps(self):
        yield self.join_core()
        for t in range(6):
            yield self.step(t)
        for t in reversed(range(self.halvings)):
            yield self.back(t)

    def finish(self):
        self.wait_bytes(self.half, self.fwd_send.at[self.r], self.fwd_recv.at[self.r])


def out_slices(blk, gqkv, gout, gup, gdown):
    cols = [pl.ds(c * D, D) for c in range(4)]
    return ([gqkv.at[blk, :, cols[c]] for c in range(3)] + [gout.at[blk]] + [gup.at[blk, :, cols[c]] for c in range(4)]
            + [gdown.at[blk, cols[c]] for c in range(4)])


def step_kernel(n, x_hbm, cot_hbm, ln_in, wqkv_hbm, wout_hbm, wup_hbm, wdown_hbm,
                y_ref, dx_ref, gln_ref, grads,
                x_s, cot_s, mid_s, dmid_s, h_s, ln_s, wqkv, wout, wup, wdown, qkv_s, p_s, o_s,
                m_s, act_s, dup_s, dhid_s, datt_s, dqkv_s, a_s, m0_s, act0_s, snd, rcv, lnacc, lnrecv, *rest):
    halves, recvs = rest[:ROUNDS], rest[ROUNDS:2 * ROUNDS]
    (load_sem, swap_send, swap_recv, swap_local, *sems) = rest[2 * ROUNDS:]
    me = lax.axis_index("sp")
    dims = [dim_info(me, d) for d in range(6)]
    sibling = me + 1 - 2 * lax.rem(me, 2)
    ln_send, ln_recv = sems[-2:]
    sems = sems[:-2]

    loads = {}
    for name, src, dst in (("x", x_hbm, x_s), ("qkv0", wqkv_hbm.at[0], wqkv.at[0]), ("cot", cot_hbm, cot_s),
                           ("out0", wout_hbm.at[0], wout.at[0]), ("up0", wup_hbm.at[0], wup.at[0]),
                           ("down0", wdown_hbm.at[0], wdown.at[0]), ("qkv1", wqkv_hbm.at[1], wqkv.at[1]),
                           ("out1", wout_hbm.at[1], wout.at[1]), ("up1", wup_hbm.at[1], wup.at[1]),
                           ("down1", wdown_hbm.at[1], wdown.at[1])):
        loads[name] = pltpu.make_async_copy(src, dst, load_sem.at[len(loads)])
        loads[name].start()

    barrier = pltpu.get_barrier_semaphore()

    def greet_one(k):
        pl.semaphore_signal(barrier, inc=1, device_id={"sp": lax.rem(me + k, n)}, device_id_type=MESH)

    def greet(k, _):
        for j in range(4):
            greet_one(4 * k + 1 + j)
        return 0
    lax.fori_loop(0, (n - 1) // 4, greet, 0)
    for k in range((n - 1) // 4 * 4 + 1, n):
        greet_one(k)

    def need(*names):
        for name in names:
            loads[name].wait()

    def remote_piece(i, k):
        to = lax.rem(me + k, n)
        return remote_copy(snd.at[i % 2, to], rcv.at[i, me], swap_send.at[i], swap_recv.at[i], to)

    def start_swap(i):
        pltpu.make_async_copy(snd.at[i % 2, me], rcv.at[i, me], swap_local.at[i]).start()

        def send(k, _):
            for j in range(4):
                remote_piece(i, 4 * k + 1 + j).start()
            return 0
        lax.fori_loop(0, (n - 1) // 4, send, 0)
        for k in range((n - 1) // 4 * 4 + 1, n):
            remote_piece(i, k).start()

    def end_swap(i):
        pltpu.make_async_copy(snd.at[i % 2, me], rcv.at[i, me], swap_local.at[i]).wait()
        rest = pl.ds(0, n - 1)
        pltpu.make_async_copy(snd.at[i % 2, rest], rcv.at[i, rest], swap_send.at[i]).wait()
        pltpu.make_async_copy(snd.at[i % 2, rest], rcv.at[i, rest], swap_recv.at[i]).wait()

    ln_s[...] = ln_in[...].astype(F32)
    lnacc[...] = jnp.zeros_like(lnacc)
    ln = [ln_s.at[i] for i in range(2)]
    lng = [lnacc.at[pl.ds(8 * i, 8)] for i in range(2)]
    saved = [(qkv_s.at[i], p_s.at[i], o_s.at[i]) for i in range(2)]
    rounds = [Round(r, grads, me, dims, halves[r], recvs[r], sems) for r in range(ROUNDS)]
    r1, r2, r3, r4 = rounds

    def ln_copy(t):
        to = sibling if t == 0 else dims[t - 1][1]
        return remote_copy(lnacc, lnrecv.at[t], ln_send.at[0], ln_recv.at[t], to)

    def ln_next(t):
        ln_copy(t).wait()
        lnacc[...] += lnrecv[t]
        if t < 6:
            ln_copy(t + 1).start()

    def ln_steps():
        for t in range(7):
            yield ln_next(t)

    walks = [rnd.steps() for rnd in rounds] + [ln_steps()]

    def slot(name):
        for digit in SCHEDULE[name]:
            next(walks[int(digit) - 1])

    need("x", "qkv0")
    attn_forward(x_s, ln[0], wqkv.at[0], *saved[0])
    need("cot")
    to_pieces(cot_s, snd.at[0])
    need("out0", "up0", "down0")
    h_s[...] = hidden(x_s, o_s.at[0], wout.at[0])
    mid_s[...] = mlp_forward(h_s[...].astype(F32), ln[0], wup.at[0], wdown.at[0], act0_s)
    to_pieces(mid_s, snd.at[1])
    pl.semaphore_wait(barrier, n - 1)
    start_swap(1)
    start_swap(0)
    slopes = grads.at[0]
    mlp_prepare(h_s, ln[0], wup.at[0], m0_s, act0_s, slopes)

    need("qkv1", "out1", "up1", "down1")
    end_swap(1)
    from_pieces(rcv.at[1], mid_s)
    attn_forward(mid_s, ln[1], wqkv.at[1], *saved[1])
    end_swap(0)
    from_pieces(rcv.at[0], cot_s)
    mlp_both_ways(hidden(mid_s, o_s.at[1], wout.at[1]).astype(F32), cot_s, ln[1], wup.at[1], wout.at[1], wdown.at[1], m_s, act_s,
                  dup_s, dhid_s, datt_s, lng[1], y_ref)
    to_pieces(y_ref, snd.at[0])
    start_swap(2)
    mlp_grads_first(grads.at[1], m_s, act_s, dup_s, cot_s)
    r1.start_core()
    slot("b")
    attn_backward(qkv_s.at[1], p_s.at[1], datt_s, dqkv_s, lambda: slot("c0"))
    slot("c1")
    qkv_backward(mid_s, dqkv_s, dhid_s, ln[1], wqkv.at[1], a_s, dmid_s, lng[1])
    to_pieces(dmid_s, snd.at[1])
    start_swap(3)
    mlp_grads_last(grads.at[1], act_s, dhid_s, o_s.at[1], cot_s)
    qkv_grads(grads.at[1], a_s, dqkv_s)
    r2.start_core()
    slot("e")
    end_swap(2)
    from_pieces(rcv.at[2], y_ref)
    slot("f")
    end_swap(3)
    from_pieces(rcv.at[3], dmid_s)

    mlp_backward(h_s, dmid_s, slopes, ln[0], wup.at[0], wout.at[0], wdown.at[0], dup_s, dhid_s, datt_s, lng[0],
                 lambda: slot("h0"))
    slot("h1")
    mlp_grads_first(grads.at[0], m0_s, act0_s, dup_s, dmid_s)
    r3.start_core()
    slot("i")
    mlp_grads_last(grads.at[0], act0_s, dhid_s, o_s.at[0], dmid_s)
    slot("j")
    attn_backward(qkv_s.at[0], p_s.at[0], datt_s, dqkv_s, lambda: slot("k0"))
    slot("k1")
    qkv_backward(x_s, dqkv_s, dhid_s, ln[0], wqkv.at[0], a_s, dx_ref, lng[0])
    ln_copy(0).start()
    slot("l")
    qkv_grads(grads.at[0], a_s, dqkv_s)
    r4.start_core()
    slot("tail")
    for rnd in rounds:
        rnd.finish()
    for i in range(2):
        gln_ref[i] = lnacc[8 * i:8 * i + 4, :]


def publish_kernel(y_in, dx_in, gln_in, grads, y_ref, dx_ref, gln_ref, gqkv, gout, gup, gdown, sem):
    pairs = [(y_in, y_ref), (dx_in, dx_ref), (gln_in, gln_ref)]
    for i in range(2):
        slices = out_slices(i, gqkv, gout, gup, gdown)
        pairs += [(grads.at[i, j], slices[j]) for j in range(12)]
    copies = [pltpu.make_async_copy(src, dst, sem.at[k]) for k, (src, dst) in enumerate(pairs)]
    for copy in copies:
        copy.start()
    for copy in copies:
        copy.wait()


def device_step(n, latents, cotangent, ln_params, w_qkv, w_out, w_up, w_down):
    dma = pltpu.SemaphoreType.DMA
    regular = pltpu.SemaphoreType.REGULAR
    any_spec = pl.BlockSpec(memory_space=pl.ANY)
    vmem_spec = pl.BlockSpec(memory_space=pltpu.VMEM)
    act, wide, qkv = (T, D), (T, FF), (T, 3 * D)
    shapes = [(act, BF16), (act, BF16), ((2, 4, D), F32)]
    held = pl.pallas_call(
        functools.partial(step_kernel, n),
        out_shape=[pltpu.VMEM(s, t) for s, t in shapes] + [pltpu.VMEM((2, 12, D, D), F32)],
        in_specs=[any_spec, any_spec, vmem_spec] + [any_spec] * 4,
        out_specs=[vmem_spec] * 4,
        scratch_shapes=[pltpu.VMEM(s, BF16) for s in [act] * 5]
        + [pltpu.VMEM((2, 4, D), F32)]
        + [pltpu.VMEM((2,) + s, BF16) for s in ((D, 3 * D), (D, D), (D, FF), (FF, D), qkv, (12, SEQ, SEQ), act)]
        + [pltpu.VMEM(s, BF16) for s in (act, wide, wide, act, act, qkv, act, act, wide)]
        + [pltpu.VMEM((2, n, 2, 2, D), BF16), pltpu.VMEM((4, n, 2, 2, D), BF16)]
        + [pltpu.VMEM((16, D), F32), pltpu.VMEM((7, 16, D), F32)]
        + [pltpu.VMEM((6, round_sizes(blocks)[0], D), F32) for blocks in ROUND_BLOCKS]
        + [pltpu.VMEM((6, sum(round_sizes(blocks)[2]), D), F32) for blocks in ROUND_BLOCKS]
        + [dma((10,)), dma((4,)), dma((4,)), dma((4,))]
        + [dma((ROUNDS,))] * 3 + [dma((ROUNDS, 6)), dma((ROUNDS,)), dma((ROUNDS, 3)), dma((ROUNDS,)), dma((ROUNDS,))]
        + [regular((ROUNDS, 3)), regular((ROUNDS,)), dma((1,)), dma((7,))],
        compiler_params=pltpu.CompilerParams(collective_id=0, has_side_effects=True, vmem_limit_bytes=STEP_VMEM),
        cost_estimate=pl.CostEstimate(flops=12_000_000_000, bytes_accessed=30_000_000, transcendentals=0),
    )(latents.reshape(T, D), cotangent.reshape(T, D), ln_params, w_qkv, w_out.reshape(2, D, D), w_up, w_down)
    y, dx, gln, gqkv, gout, gup, gdown = pl.pallas_call(
        publish_kernel,
        out_shape=[jax.ShapeDtypeStruct(s, t) for s, t in shapes]
        + [jax.ShapeDtypeStruct(s, F32) for s in ((2, D, 3 * D), (2, D, D), (2, D, FF), (2, FF, D))],
        in_specs=[vmem_spec] * 4,
        out_specs=[any_spec] * 7,
        scratch_shapes=[dma((27,))],
        compiler_params=pltpu.CompilerParams(vmem_limit_bytes=2_000_000),
    )(*held)
    return (y.reshape(latents.shape), dx.reshape(latents.shape), gln, gqkv, gout.reshape(2, 6, 64, D), gup, gdown)


def solution(mesh):
    act_spec = P('data', 'sp', None, None)
    replicated = P()
    part_spec = P('data')
    return jax.shard_map(functools.partial(device_step, mesh.shape["sp"]), mesh=mesh,
                         in_specs=(act_spec, act_spec, replicated, replicated, replicated, replicated, replicated),
                         out_specs=(act_spec, act_spec, part_spec, part_spec, part_spec, part_spec, part_spec),
                         check_vma=False)
```
